128 devices in a mesh: problem: 1, samp: 16 (over z, y), feat: 8 (over x, core).
Axes of the slice: x: 4, y: 4, z: 4, core: 2. Of those that a mesh axis runs over, the one named last changes fastest.
Arguments:
- design: bfloat16 [8192, 65536], P(('problem', 'samp'), 'feat')
- targets: float32 [8192, 128], P(('problem', 'samp'))
- coef_init: float32 [65536, 128], P(('problem', 'feat'))
- step_sizes: float32 [65536], P(('problem', 'feat'))
- ridge_weights: float32 [128], P('problem')
Outputs:
- output 1: float32 [65536, 128], P(('problem', 'feat'))
- output 2: float32 [8192, 128], P(('problem', 'samp'))
All inputs are finite; a program needn't handle non-finite values.
Results may differ from the reference program's by a relative error of at most 0.00675681.
Values are sent between devices in bfloat16 or wider.
A program may use at most 1 GiB of HBM per device.

```python
import jax
import jax.numpy as jnp
from jax import lax

NUM_ROWS = 8192
NUM_FEATURES = 65536
NUM_TARGETS = 128
FEAT_BLOCKS = 8
SWEEPS = 4
STEP_WEIGHT = 0.5


def setup_inputs(seed: int = 0, part: int = 0) -> dict:
    base_key = jax.random.fold_in(jax.random.key(seed), part)
    sub_keys = jax.random.split(base_key, 9)
    shared_rank = 8
    shared_mix = 0.8
    row_block = NUM_ROWS // 8
    factors = jax.random.normal(sub_keys[0], (NUM_ROWS, shared_rank), jnp.float32)
    loadings = jax.random.normal(sub_keys[1], (shared_rank, NUM_FEATURES), jnp.float32)

    def draw_rows(block_index):
        rows_f = lax.dynamic_slice_in_dim(factors, block_index * row_block, row_block, 0)
        shared = jnp.dot(rows_f, loadings) * (shared_mix / shared_rank) ** 0.5
        noise_blk = jax.random.normal(jax.random.fold_in(sub_keys[2], block_index), (row_block, NUM_FEATURES), jnp.float32)
        return (shared + (1.0 - shared_mix) ** 0.5 * noise_blk).astype(jnp.bfloat16)

    design = lax.map(draw_rows, jnp.arange(8)).reshape(NUM_ROWS, NUM_FEATURES)

    def power_step(step_index, probe_vec):
        unit_vec = probe_vec / jnp.linalg.norm(probe_vec)
        image_vec = jnp.dot(design, unit_vec.astype(jnp.bfloat16), preferred_element_type=jnp.float32)
        return jnp.dot(image_vec.astype(jnp.bfloat16), design, preferred_element_type=jnp.float32) / NUM_ROWS

    probe_init = jax.random.normal(sub_keys[3], (NUM_FEATURES,), jnp.float32)
    curvature = 1.15 * jnp.linalg.norm(lax.fori_loop(0, 12, power_step, probe_init))
    step_sizes = jax.random.uniform(sub_keys[4], (NUM_FEATURES,), jnp.float32, 0.4, 0.8) / curvature
    ridge_weights = jax.random.uniform(sub_keys[5], (NUM_TARGETS,), jnp.float32, 0.05, 0.25) * curvature
    coef_init = jax.random.normal(sub_keys[6], (NUM_FEATURES, NUM_TARGETS), jnp.float32) * NUM_FEATURES ** -0.5
    w_star = jax.random.normal(sub_keys[7], (NUM_FEATURES, NUM_TARGETS), jnp.float32) * NUM_FEATURES ** -0.5
    targets = jnp.dot(design, w_star.astype(jnp.bfloat16), preferred_element_type=jnp.float32) + 0.3 * jax.random.normal(sub_keys[8], (NUM_ROWS, NUM_TARGETS), jnp.float32)
    return {"design": design, "targets": targets, "coef_init": coef_init, "step_sizes": step_sizes, "ridge_weights": ridge_weights}


def reference(design, targets, coef_init, step_sizes, ridge_weights):
    block_cols = NUM_FEATURES // FEAT_BLOCKS

    def block_sum(weights):
        weights_b = weights.astype(jnp.bfloat16)

        def add_block(acc_sum, block_index):
            col_block = lax.dynamic_slice_in_dim(design, block_index * block_cols, block_cols, 1)
            rows_w = lax.dynamic_slice_in_dim(weights_b, block_index * block_cols, block_cols, 0)
            product = jnp.dot(col_block, rows_w, preferred_element_type=jnp.float32)
            return acc_sum + product.astype(jnp.bfloat16).astype(jnp.float32), None

        return lax.scan(add_block, jnp.zeros((NUM_ROWS, NUM_TARGETS), jnp.float32), jnp.arange(FEAT_BLOCKS))[0]

    def sweep_once(sweep_state, unused):
        coef_cur, resid_cur = sweep_state
        gradient = lax.dot_general(design, resid_cur.astype(jnp.bfloat16), (((0,), (0,)), ((), ())), preferred_element_type=jnp.float32) / NUM_ROWS
        step_delta = step_sizes[:, None] * (gradient - ridge_weights[None, :] * coef_cur)
        return (coef_cur + STEP_WEIGHT * step_delta, resid_cur - STEP_WEIGHT * block_sum(step_delta)), None

    start_state = (coef_init, targets - block_sum(coef_init))
    final_state = lax.scan(sweep_once, start_state, None, length=SWEEPS)[0]
    return final_state[0], final_state[1]
```

```python
import jax
import jax.numpy as jnp
from jax import lax
from jax.experimental import pallas as pl
from jax.experimental.pallas import tpu as pltpu
from jax.sharding import PartitionSpec as P

SWEEPS = 4
STEP_WEIGHT = 0.5
RING = 4
FEATS = 8
LANES = 128
ORDER = (2, 1, 3, 0)
STREAMS = 2
MESH_ID = pl.DeviceIdType.MESH
AG_MSGS = 22
F32 = jnp.float32
BF16 = jnp.bfloat16


def merge(first, second):
    live = [first, second]
    while live:
        for gen in list(live):
            try:
                next(gen)
            except StopIteration:
                live.remove(gen)


def run(gen):
    for _ in gen:
        pass


def make_kernel(total_rows, tgt):
    half = tgt // 2
    inv_rows = 1.0 / total_rows

    def kernel(x_hbm, y_hbm, w0_hbm, eta_ref, lam_ref, w_out, r_out,
               xv, wst, yst, sg, wg, gt, fin, din, cin, f2in, d2in, c2in, wown, lamb, rt, acc,
               ub, urecv, rbuf, rown, rfin,
               xsem, wsem, ysem, osem, rs_send, rs_recv, ag_recv, x_send, u_recv, r_recv, rf_recv):
        samp = lax.axis_index("samp")
        feat = lax.axis_index("feat")
        zpos = samp // RING
        ypos = samp % RING

        def wrap(v):
            return lax.rem(v + RING, RING)

        def dev(z, y):
            return (0, z * RING + y, feat)

        z_plus, z_minus = dev(wrap(zpos + 1), ypos), dev(wrap(zpos - 1), ypos)
        y_plus, y_minus = dev(zpos, wrap(ypos + 1)), dev(zpos, wrap(ypos - 1))
        first_nbr = ((y_plus, y_minus), (z_plus, z_minus))
        second_nbr = ((z_plus, z_minus), (y_plus, y_minus))

        def place(h, o1, o2):
            if h == 0:
                return wrap(zpos + o2), wrap(ypos + o1)
            return wrap(zpos + o1), wrap(ypos + o2)

        def peer(k):
            return lax.rem(feat + k, FEATS)

        x_copies = [pltpu.make_async_copy(x_hbm.at[:, pl.ds(c * 256, 256)], xv.at[c], xsem.at[c]) for c in range(32)]
        w_copies = [pltpu.make_async_copy(w0_hbm.at[pl.ds(8 * q, 8)], wst.at[pl.ds(8 * q, 8)], wsem.at[q]) for q in range(4)]
        y_copy = pltpu.make_async_copy(y_hbm.at[pl.ds(pl.multiple_of((feat // 2) * LANES, LANES), LANES)], yst, ysem)
        w_copies[0].start()
        y_copy.start()
        for q in range(4):
            if q:
                w_copies[q].start()
            for c in range(8 * q, 8 * q + 8):
                x_copies[c].start()

        barrier = pltpu.get_barrier_semaphore()
        for nbr in (z_plus, z_minus, y_plus, y_minus):
            pl.semaphore_signal(barrier, inc=1, device_id=nbr, device_id_type=MESH_ID)
        for k in range(1, FEATS):
            pl.semaphore_signal(barrier, inc=1, device_id=(0, samp, peer(k)), device_id_type=MESH_ID)
        pl.semaphore_wait(barrier, 4 + FEATS - 1)

        def remote(src, dst, send, recv, to):
            return pltpu.make_async_remote_copy(src_ref=src, dst_ref=dst, send_sem=send, recv_sem=recv, device_id=to, device_id_type=MESH_ID)

        def rs1(t, h, kind, way, jo):
            io, pm = {"F": (2, way), "D": (1 + 2 * way, 1 - way), "C": (1 + 2 * way, way)}[kind]
            land = {"F": fin, "D": din, "C": cin}[kind]
            slot = ((h * 3 + "FDC".index(kind)) * 2 + way) * 4 + jo
            return remote(gt.at[t, h, io, jo, pm], land.at[t, h, way, jo], rs_send.at[t, slot], rs_recv.at[t, slot], first_nbr[h][way])

        def rs2(t, h, kind, way):
            jo, pm = {"F": (2, way), "D": (1 + 2 * way, 1 - way), "C": (1 + 2 * way, way)}[kind]
            land = {"F": f2in, "D": d2in, "C": c2in}[kind]
            slot = 48 + (h * 3 + "FDC".index(kind)) * 2 + way
            return remote(gt.at[t, h, 0, jo, pm], land.at[t, h, way], rs_send.at[t, slot], rs_recv.at[t, slot], second_nbr[h][way])

        def ag(t, h, idx, buf, recv):
            if idx < 2:
                to, (o1, o2), rows = second_nbr[h][idx], (0, 0), None
            elif idx < 4:
                to, (o1, o2), rows = second_nbr[h][idx - 2], (0, (-1, 1)[idx - 2]), idx - 2
            elif idx < 14:
                way, m = (idx - 4) // 5, (idx - 4) % 5
                to, o1 = first_nbr[h][way], 0
                o2, rows = ((0, None), (-1, None), (1, None), (2, 0), (2, 1))[m]
            else:
                way, m = (idx - 14) // 4, (idx - 14) % 4
                to, o1, rows = first_nbr[h][way], (-1, 1)[way], way
                o2 = (0, -1, 1, 2)[m]
            zi, yi = place(h, o1, o2)
            ref = buf.at[t, zi, yi, h] if rows is None else buf.at[t, zi, yi, h, pl.ds(rows * half, half)]
            slot = h * AG_MSGS + idx
            return remote(ref, ref, rs_send.at[t, slot], recv.at[t, slot], to)

        def gather(t, buf, recv):
            def go(h, *idxs):
                for idx in idxs:
                    ag(t, h, idx, buf, recv).start()

            def got(h, *idxs):
                for idx in idxs:
                    ag(t, h, idx, buf, recv).wait_recv()

            for h in range(2):
                go(h, 0, 1, 4, 9)
            yield
            for h in range(2):
                got(h, 0)
                go(h, 2, 5, 10)
                got(h, 1)
                go(h, 3, 6, 11)
            yield
            for h in range(2):
                got(h, 4)
                go(h, 14)
                got(h, 9)
                go(h, 18)
            yield
            for h in range(2):
                got(h, 2)
                go(h, 7, 12)
                got(h, 3)
                go(h, 8, 13)
            yield
            for h in range(2):
                got(h, 5)
                go(h, 15)
                got(h, 6)
                go(h, 16)
                got(h, 10)
                go(h, 19)
                got(h, 11)
                go(h, 20)
            yield
            for h in range(2):
                got(h, 7)
                go(h, 17)
                got(h, 13)
                go(h, 21)
            yield
            for h in range(2):
                got(h, 8, 12, *range(14, 22))
            for h in range(2):
                for idx in range(AG_MSGS):
                    ag(t, h, idx, buf, recv).wait_send()

        def samp_phase(t):
            for io in ORDER:
                for h in range(2):
                    for jo in ORDER:
                        zi, yi = place(h, io, jo)
                        res = jnp.dot(rt[t], xv[(zi * RING + yi) * 2 + h], preferred_element_type=F32)
                        gt[t, h, io, jo, 0] = res[:, :LANES]
                        gt[t, h, io, jo, 1] = res[:, LANES:]
                        if io == 2:
                            rs1(t, h, "F", 0, jo).start()
                            rs1(t, h, "F", 1, jo).start()
                        elif io:
                            rs1(t, h, "D", io // 2, jo).start()
                yield
            for jo in ORDER:
                for h in range(2):
                    for way in range(2):
                        rs1(t, h, "F", way, jo).wait_recv()
                        gt[t, h, 1 + 2 * way, jo, way] += fin[t, h, way, jo]
                        rs1(t, h, "C", way, jo).start()
                yield
            for jo in ORDER:
                for h in range(2):
                    for way in range(2):
                        rs1(t, h, "D", way, jo).wait_recv()
                        rs1(t, h, "C", way, jo).wait_recv()
                    for pm in range(2):
                        gt[t, h, 0, jo, pm] = gt[t, h, 0, jo, pm] + cin[t, h, pm, jo] + din[t, h, 1 - pm, jo]
                    if jo == 2:
                        rs2(t, h, "F", 0).start()
                        rs2(t, h, "F", 1).start()
                    elif jo:
                        rs2(t, h, "D", jo // 2).start()
                yield
            for h in range(2):
                for way in range(2):
                    rs2(t, h, "F", way).wait_recv()
                    gt[t, h, 0, 1 + 2 * way, way] += f2in[t, h, way]
                    rs2(t, h, "C", way).start()
            yield
            for h in range(2):
                for way in range(2):
                    rs2(t, h, "D", way).wait_recv()
                    rs2(t, h, "C", way).wait_recv()
                for pm in range(2):
                    grad = (gt[t, h, 0, 0, pm] + c2in[t, h, pm] + d2in[t, h, 1 - pm]) * inv_rows
                    old = wown[t, h, pm]
                    step = eta_ref[pl.ds((samp * 2 + h) * 2 + pm, 1), :] * (grad - lamb[t] * old)
                    wown[t, h, pm] = old + STEP_WEIGHT * step
                    sg[t, zpos, ypos, h, :, pl.ds(pm * LANES, LANES)] = step.astype(BF16)
            for h in range(2):
                for kind in "FDC":
                    for way in range(2):
                        for jo in range(RING):
                            rs1(t, h, kind, way, jo).wait_send()
                        rs2(t, h, kind, way).wait_send()
            yield from gather(t, sg, ag_recv)

        def xmsg(t, k, src, dst, recv):
            return remote(src, dst, x_send.at[t, k], recv.at[t, k], (0, samp, peer(k)))

        def feat_phase(t, weight, loading=False, final=False):
            for zi in range(RING):
                part = None
                for yi in range(RING):
                    for h in range(2):
                        c = (zi * RING + yi) * 2 + h
                        if loading:
                            x_copies[c].wait()
                        prod = lax.dot_general(sg[t, zi, yi, h], xv[c], (((1,), (1,)), ((), ())), preferred_element_type=F32)
                        part = prod if part is None else part + prod
                acc[t] = part if zi == 0 else acc[t] + part
                yield
            for j in range(FEATS):
                ub[t, j] = acc[t, pl.ds((j % 2) * half, half), pl.ds((j // 2) * LANES, LANES)].astype(BF16)
            for k in range(1, FEATS):
                xmsg(t, k, ub.at[t, peer(k)], urecv.at[t, feat], u_recv).start()
            urecv[t, feat] = ub[t, feat]
            yield
            for k in range(1, FEATS):
                xmsg(t, k, ub.at[t, peer(k)], urecv.at[t, feat], u_recv).wait()
            total = urecv[t, 0].astype(F32)
            for j in range(1, FEATS):
                total = total + urecv[t, j].astype(F32)
            resid = rown[t] - weight * total
            rown[t] = resid
            if final:
                return
            rbuf[t, feat] = resid.astype(BF16)
            for k in range(1, FEATS):
                xmsg(t, k, rbuf.at[t, feat], rbuf.at[t, feat], r_recv).start()
            yield
            for k in range(1, FEATS):
                xmsg(t, k, rbuf.at[t, feat], rbuf.at[t, feat], r_recv).wait()
            for j in range(FEATS):
                rt[t, pl.ds((j % 2) * half, half), pl.ds((j // 2) * LANES, LANES)] = rbuf[t, j]
            yield

        lam_cols = jnp.broadcast_to(lam_ref[...], (LANES, LANES)).T
        for t in range(STREAMS):
            lamb[t] = lam_cols[t * tgt:(t + 1) * tgt]
        y_copy.wait()
        y_cols = yst[...].T
        core = lax.rem(feat, 2)
        yst[...] = y_cols
        for t in range(STREAMS):
            rown[t] = yst[pl.ds(pl.multiple_of(t * tgt + core * half, half), half), :]
        for q in range(4):
            w_copies[q].wait()

            def flip(c, carry, q=q):
                for pm in range(2):
                    cols = wst[8 * q + c, pl.ds(pm * LANES, LANES), :].T.astype(BF16)
                    for t in range(STREAMS):
                        sg[t, q, c // 2, lax.rem(c, 2), :, pl.ds(pm * LANES, LANES)] = cols[t * tgt:(t + 1) * tgt]
                return carry

            lax.fori_loop(0, 8, flip, 0)
        for h in range(2):
            for pm in range(2):
                cols = wst[samp * 2 + h, pl.ds(pm * LANES, LANES), :].T
                for t in range(STREAMS):
                    wown[t, h, pm] = cols[t * tgt:(t + 1) * tgt]

        run(feat_phase(0, 1.0, loading=True))

        def sweep(k, carry):
            weight = jnp.where(k == 0, 1.0, STEP_WEIGHT).astype(F32)
            merge(samp_phase(0), feat_phase(1, weight))
            merge(feat_phase(0, STEP_WEIGHT), samp_phase(1))
            return carry

        lax.fori_loop(0, SWEEPS, sweep, 0)

        def finish(t):
            for h in range(2):
                for pm in range(2):
                    wg[t, zpos, ypos, h, :, pl.ds(pm * LANES, LANES)] = wown[t, h, pm]
            yield from gather(t, wg, rs_recv)

        def rmsg(t, k):
            return xmsg(t, k, rfin.at[t, feat], rfin.at[t, feat], rf_recv)

        def residual():
            rfin[0, feat] = rown[0]
            for k in range(1, FEATS):
                rmsg(0, k).start()
            yield from feat_phase(1, STEP_WEIGHT, final=True)
            rfin[1, feat] = rown[1]
            for k in range(1, FEATS):
                rmsg(1, k).start()
            yield
            for t in range(STREAMS):
                for k in range(1, FEATS):
                    rmsg(t, k).wait()

        def both():
            merge_steps = [finish(0), finish(1)]
            while merge_steps:
                for gen in list(merge_steps):
                    try:
                        next(gen)
                    except StopIteration:
                        merge_steps.remove(gen)
                yield

        merge(both(), residual())
        w_done = pltpu.make_async_copy(wg, w_out, osem.at[0])
        r_done = pltpu.make_async_copy(rfin, r_out, osem.at[1])
        w_done.start()
        r_done.start()
        w_done.wait()
        r_done.wait()

    return kernel


def solution(mesh):
    samp_size = mesh.shape["samp"]
    design_spec = P(("problem", "samp"), "feat")
    rows_spec = P(("problem", "samp"), None)
    coef_spec = P(("problem", "feat"), None)
    step_spec = P(("problem", "feat"))
    ridge_spec = P("problem")

    def local(design, targets, coef_init, step_sizes, ridge_weights):
        rows, cols = design.shape
        n_tgt = targets.shape[1]
        tgt = n_tgt // STREAMS
        half = tgt // 2
        own = (STREAMS, RING, RING, 2, tgt, 256)
        vm = pltpu.VMEM
        dma = pltpu.SemaphoreType.DMA
        any_spec = pl.BlockSpec(memory_space=pl.ANY)
        vmem_spec = pl.BlockSpec(memory_space=pltpu.VMEM)
        w_t, r_t = pl.pallas_call(
            make_kernel(rows * samp_size, tgt),
            out_shape=(jax.ShapeDtypeStruct(own, F32), jax.ShapeDtypeStruct((STREAMS, FEATS, half, LANES), F32)),
            in_specs=[any_spec, any_spec, any_spec, vmem_spec, vmem_spec],
            out_specs=(any_spec, any_spec),
            scratch_shapes=[
                vm((32, rows, 256), BF16),
                vm((32, 256, LANES), F32),
                vm((LANES, LANES), F32),
                vm(own, BF16),
                vm(own, F32),
                vm((STREAMS, 2, RING, RING, 2, tgt, LANES), F32),
                vm((STREAMS, 2, 2, RING, tgt, LANES), F32),
                vm((STREAMS, 2, 2, RING, tgt, LANES), F32),
                vm((STREAMS, 2, 2, RING, tgt, LANES), F32),
                vm((STREAMS, 2, 2, tgt, LANES), F32),
                vm((STREAMS, 2, 2, tgt, LANES), F32),
                vm((STREAMS, 2, 2, tgt, LANES), F32),
                vm((STREAMS, 2, 2, tgt, LANES), F32),
                vm((STREAMS, tgt, LANES), F32),
                vm((STREAMS, tgt, rows), BF16),
                vm((STREAMS, tgt, rows), F32),
                vm((STREAMS, FEATS, half, LANES), BF16),
                vm((STREAMS, FEATS, half, LANES), BF16),
                vm((STREAMS, FEATS, half, LANES), BF16),
                vm((STREAMS, half, LANES), F32),
                vm((STREAMS, FEATS, half, LANES), F32),
                dma((32,)),
                dma((4,)),
                dma,
                dma((2,)),
                dma((STREAMS, 60)),
                dma((STREAMS, 60)),
                dma((STREAMS, 44)),
                dma((STREAMS, FEATS)),
                dma((STREAMS, FEATS)),
                dma((STREAMS, FEATS)),
                dma((STREAMS, FEATS)),
            ],
            compiler_params=pltpu.CompilerParams(collective_id=0, has_side_effects=True, vmem_limit_bytes=60 * 1024 * 1024),
        )(design, targets, coef_init.reshape(32, 256, n_tgt), step_sizes.reshape(cols // LANES, LANES), ridge_weights.reshape(1, n_tgt))
        coef = w_t.transpose(1, 2, 3, 5, 0, 4).reshape(cols, n_tgt)
        resid = r_t.reshape(STREAMS, RING, 2, half, LANES).transpose(1, 4, 0, 2, 3).reshape(rows, n_tgt)
        return coef, resid

    return jax.shard_map(local, mesh=mesh, in_specs=(design_spec, rows_spec, coef_spec, step_spec, ridge_spec), out_specs=(coef_spec, rows_spec), check_vma=False)
```

```python
import jax
import jax.numpy as jnp
from jax import lax
from jax.experimental import pallas as pl
from jax.experimental.pallas import tpu as pltpu
from jax.sharding import PartitionSpec as P

SWEEPS = 4
STEP_WEIGHT = 0.5
RING = 4
FEATS = 8
LANES = 128
ORDER = (2, 1, 3, 0)
STREAMS = 2
MESH_ID = pl.DeviceIdType.MESH
AG_MSGS = 19
RS_MSGS = 26
FIRST = ""
ORDER_AB = "1"
ORDER_END = ""
F32 = jnp.float32
BF16 = jnp.bfloat16


def weave(order, *gens):
    live = dict(enumerate(gens))

    def step(i):
        if i in live:
            try:
                next(live[i])
            except StopIteration:
                del live[i]

    for ch in order:
        step(int(ch))
    while live:
        for i in sorted(live):
            step(i)


def run(gen):
    for _ in gen:
        pass


def make_kernel(total_rows, tgt):
    half = tgt // 2
    inv_rows = 1.0 / total_rows

    def kernel(x_hbm, y_hbm, w0_hbm, eta_ref, lam_ref, w_out, r_out,
               xv, wst, yst, rnat, flat, sg, wg, gt, fin, din, cin, r2in, wown, lamb, rt, acc,
               ub, urecv, rbuf, rown, rfin,
               xsem, wsem, ysem, rs_send, rs_recv, ag_recv, w_send, w_recv, x_send, u_recv, r_recv, rf_recv):
        samp = lax.axis_index("samp")
        feat = lax.axis_index("feat")
        zpos = samp // RING
        ypos = samp % RING

        def wrap(v):
            return lax.rem(v + RING, RING)

        def dev(z, y):
            return (0, z * RING + y, feat)

        z_plus, z_minus = dev(wrap(zpos + 1), ypos), dev(wrap(zpos - 1), ypos)
        y_plus, y_minus = dev(zpos, wrap(ypos + 1)), dev(zpos, wrap(ypos - 1))
        first_nbr = ((y_plus, y_minus), (z_plus, z_minus))
        second_nbr = ((z_plus, z_minus), (y_plus, y_minus))

        def place(h, o1, o2):
            if h == 0:
                return wrap(zpos + o2), wrap(ypos + o1)
            return wrap(zpos + o1), wrap(ypos + o2)

        def peer(k):
            return lax.rem(feat + k, FEATS)

        x_copies = [pltpu.make_async_copy(x_hbm.at[:, pl.ds(c * 256, 256)], xv.at[c], xsem.at[c]) for c in range(32)]
        w_copy = pltpu.make_async_copy(w0_hbm.at[pl.ds(samp * 2, 2)], wst.at[pl.ds(0, 2)], wsem.at[0])
        y_copy = pltpu.make_async_copy(y_hbm.at[pl.ds(pl.multiple_of((feat // 2) * LANES, LANES), LANES)], yst, ysem)
        w_copy.start()
        y_copy.start()
        for copy in x_copies:
            copy.start()

        barrier = pltpu.get_barrier_semaphore()
        for nbr in (z_plus, z_minus, y_plus, y_minus, dev(wrap(zpos + 2), ypos), dev(zpos, wrap(ypos + 2))):
            pl.semaphore_signal(barrier, inc=1, device_id=nbr, device_id_type=MESH_ID)
        for k in range(1, FEATS):
            pl.semaphore_signal(barrier, inc=1, device_id=(0, samp, peer(k)), device_id_type=MESH_ID)
        pl.semaphore_wait(barrier, 6 + FEATS - 1)

        def remote(src, dst, send, recv, to):
            return pltpu.make_async_remote_copy(src_ref=src, dst_ref=dst, send_sem=send, recv_sem=recv, device_id=to, device_id_type=MESH_ID)

        def rs1(t, h, kind, way, part):
            io, pm = {"F": (2, way), "D": (1 + 2 * way, 1 - way), "C": (1 + 2 * way, way)}[kind]
            land = {"F": fin, "D": din, "C": cin}[kind]
            rows = pl.ds(0, 4) if kind == "D" else pl.ds(2 * part, 2)
            slot = (h * 2 + way) * 5 + {"F": part, "C": 2 + part, "D": 4}[kind]
            return remote(gt.at[t, h, io, pm, rows], land.at[t, h, way, rows], rs_send.at[t, slot], rs_recv.at[t, slot], first_nbr[h][way])

        def rs2(t, h, js):
            jo = ORDER[js]
            slot = 20 + h * 3 + js
            zi, yi = place(h, 0, jo)
            return remote(gt.at[t, h, 0, :, js], r2in.at[t, h, js], rs_send.at[t, slot], rs_recv.at[t, slot], dev(zi, yi))

        def ag(t, h, idx, buf, send, recv):
            if idx < 3:
                (o1, o2), rows = (0, 0), None
                to = dev(*place(h, 0, ORDER[idx]))
            elif idx < 11:
                way, m = (idx - 3) // 4, (idx - 3) % 4
                to, o1, rows = first_nbr[h][way], 0, None
                o2 = (0, -1, 1, 2)[m]
            else:
                way, m = (idx - 11) // 4, (idx - 11) % 4
                to, o1, rows = first_nbr[h][way], (-1, 1)[way], way
                o2 = (0, -1, 1, 2)[m]
            zi, yi = place(h, o1, o2)
            ref = buf.at[t, zi, yi, h] if rows is None else buf.at[t, zi, yi, h, pl.ds(rows * half, half)]
            slot = h * AG_MSGS + idx
            return remote(ref, ref, send.at[t, slot], recv.at[t, slot], to)

        def gather(t, buf, send, recv, work=None):
            def go(h, *idxs):
                for idx in idxs:
                    ag(t, h, idx, buf, send, recv).start()

            def got(h, *idxs):
                for idx in idxs:
                    ag(t, h, idx, buf, send, recv).wait_recv()

            for h in range(2):
                go(h, 0, 1, 2, 3, 7)
            yield
            for h in range(2):
                got(h, 1)
                go(h, 4, 8)
                got(h, 2)
                go(h, 5, 9)
                got(h, 0)
                go(h, 6, 10)
            yield
            if work:
                work(0)
                yield
            for h in range(2):
                got(h, 3)
                go(h, 11)
                got(h, 7)
                go(h, 15)
            yield
            for h in range(2):
                for m in range(1, 4):
                    got(h, 3 + m)
                    go(h, 11 + m)
                    got(h, 7 + m)
                    go(h, 15 + m)
            yield
            if work:
                work(-1)
                yield
                work(1)
                yield
            for h in range(2):
                got(h, *range(11, 19))
            if work:
                work(2)
            for h in range(2):
                for idx in range(AG_MSGS):
                    ag(t, h, idx, buf, send, recv).wait_send()

        def samp_phase(t):
            for io in ORDER:
                for h in range(2):
                    for js in range(RING):
                        zi, yi = place(h, io, ORDER[js])
                        res = jnp.dot(rt[t], xv[(zi * RING + yi) * 2 + h], preferred_element_type=F32)
                        gt[t, h, io, 0, js] = res[:, :LANES]
                        gt[t, h, io, 1, js] = res[:, LANES:]
                        if io == 2 and js % 2:
                            rs1(t, h, "F", 0, js // 2).start()
                            rs1(t, h, "F", 1, js // 2).start()
                    if io % 2:
                        rs1(t, h, "D", io // 2, 0).start()
                yield
            for part in range(2):
                rows = pl.ds(2 * part, 2)
                for h in range(2):
                    for way in range(2):
                        rs1(t, h, "F", way, part).wait_recv()
                        gt[t, h, 1 + 2 * way, way, rows] += fin[t, h, way, rows]
                        rs1(t, h, "C", way, part).start()
                yield
            for part in range(2):
                for h in range(2):
                    for way in range(2):
                        if part == 0:
                            rs1(t, h, "D", way, 0).wait_recv()
                        rs1(t, h, "C", way, part).wait_recv()
                    for js in range(2 * part, 2 * part + 2):
                        for pm in range(2):
                            gt[t, h, 0, pm, js] = gt[t, h, 0, pm, js] + cin[t, h, pm, js] + din[t, h, 1 - pm, js]
                        if js < 3:
                            rs2(t, h, js).start()
                yield
            for h in range(2):
                for js in range(3):
                    rs2(t, h, js).wait_recv()
                for pm in range(2):
                    grad = (gt[t, h, 0, pm, 3] + r2in[t, h, 0, pm] + r2in[t, h, 1, pm] + r2in[t, h, 2, pm]) * inv_rows
                    old = wown[t, h, pm]
                    step = eta_ref[pl.ds((samp * 2 + h) * 2 + pm, 1), :] * (grad - lamb[t] * old)
                    wown[t, h, pm] = old + STEP_WEIGHT * step
                    sg[t, zpos, ypos, h, :, pl.ds(pm * LANES, LANES)] = step.astype(BF16)
            for h in range(2):
                for way in range(2):
                    rs1(t, h, "D", way, 0).wait_send()
                    for part in range(2):
                        rs1(t, h, "F", way, part).wait_send()
                        rs1(t, h, "C", way, part).wait_send()
                for js in range(3):
                    rs2(t, h, js).wait_send()

        def xmsg(t, k, src, dst, recv):
            return remote(src, dst, x_send.at[t, k], recv.at[t, k], (0, samp, peer(k)))

        def feat_phase(t, weight, loading=False, final=False):
            def work(o1):
                if loading and o1 == 0:
                    for copy in x_copies:
                        copy.wait()
                part = None
                for h in range(2):
                    for o2 in (0, -1, 1, 2):
                        zi, yi = place(h, o1, o2)
                        c = (zi * RING + yi) * 2 + h
                        prod = lax.dot_general(sg[t, zi, yi, h], xv[c], (((1,), (1,)), ((), ())), preferred_element_type=F32)
                        part = prod if part is None else part + prod
                acc[t] = part if o1 == 0 else acc[t] + part

            yield from gather(t, sg, rs_send, ag_recv, work)
            for j in range(FEATS):
                ub[t, j] = acc[t, pl.ds((j % 2) * half, half), pl.ds((j // 2) * LANES, LANES)].astype(BF16)
            for k in range(1, FEATS):
                xmsg(t, k, ub.at[t, peer(k)], urecv.at[t, feat], u_recv).start()
            urecv[t, feat] = ub[t, feat]
            yield
            for k in range(1, FEATS):
                xmsg(t, k, ub.at[t, peer(k)], urecv.at[t, feat], u_recv).wait()
            total = urecv[t, 0].astype(F32)
            for j in range(1, FEATS):
                total = total + urecv[t, j].astype(F32)
            resid = rown[t] - weight * total
            rown[t] = resid
            if final:
                return
            rbuf[t, feat] = resid.astype(BF16)
            for k in range(1, FEATS):
                xmsg(t, k, rbuf.at[t, feat], rbuf.at[t, feat], r_recv).start()
            yield
            for k in range(1, FEATS):
                xmsg(t, k, rbuf.at[t, feat], rbuf.at[t, feat], r_recv).wait()
            for j in range(FEATS):
                rt[t, pl.ds((j % 2) * half, half), pl.ds((j // 2) * LANES, LANES)] = rbuf[t, j]
            yield

        lam_cols = jnp.broadcast_to(lam_ref[...], (LANES, LANES)).T
        for t in range(STREAMS):
            lamb[t] = lam_cols[t * tgt:(t + 1) * tgt]
        y_copy.wait()
        y_cols = yst[...].T
        core = lax.rem(feat, 2)
        yst[...] = y_cols
        for t in range(STREAMS):
            rown[t] = yst[pl.ds(pl.multiple_of(t * tgt + core * half, half), half), :]
        w_copy.wait()
        for h in range(2):
            for pm in range(2):
                cols = wst[h, pl.ds(pm * LANES, LANES), :].T
                for t in range(STREAMS):
                    mine = cols[t * tgt:(t + 1) * tgt]
                    wown[t, h, pm] = mine
                    sg[t, zpos, ypos, h, :, pl.ds(pm * LANES, LANES)] = mine.astype(BF16)

        run(feat_phase(0, 1.0, loading=True))

        def sweep(k, carry):
            weight = jnp.where(k == 0, 1.0, STEP_WEIGHT).astype(F32)
            weave(ORDER_AB, samp_phase(0), feat_phase(1, weight))
            weave(ORDER_AB, samp_phase(1), feat_phase(0, STEP_WEIGHT))
            return carry

        lax.fori_loop(0, SWEEPS, sweep, 0)

        def coef_out(t):
            for h in range(2):
                for pm in range(2):
                    wg[t, zpos, ypos, h, :, pl.ds(pm * LANES, LANES)] = wown[t, h, pm]
            yield from gather(t, wg, w_send, w_recv)

        def rmsg(t, k):
            return xmsg(t, k, rfin.at[t, feat], rfin.at[t, feat], rf_recv)

        def last(t):
            yield from feat_phase(t, STEP_WEIGHT, final=True)
            rfin[t, feat] = rown[t]
            for k in range(1, FEATS):
                rmsg(t, k).start()
            yield
            for k in range(1, FEATS):
                rmsg(t, k).wait()

        rfin[0, feat] = rown[0]
        for k in range(1, FEATS):
            rmsg(0, k).start()
        weave(ORDER_END, last(1), coef_out(0), coef_out(1))
        for k in range(1, FEATS):
            rmsg(0, k).wait()

        for q in range(4):
            def flop(c, carry, q=q):
                for pm in range(2):
                    for t in range(STREAMS):
                        flat[pm, t * tgt:(t + 1) * tgt] = wg[t, q, c // 2, lax.rem(c, 2), :, pl.ds(pm * LANES, LANES)]
                for pm in range(2):
                    wst[8 * q + c, pl.ds(pm * LANES, LANES), :] = flat[pm].T
                return carry

            lax.fori_loop(0, 8, flop, 0)
            pltpu.make_async_copy(wst.at[pl.ds(8 * q, 8)], w_out.at[pl.ds(8 * q, 8)], wsem.at[q]).start()
        for xc in range(4):
            for t in range(STREAMS):
                for core_id in range(2):
                    flat[xc % 2, pl.ds(t * tgt + core_id * half, half), :] = rfin[t, 2 * xc + core_id]
            rnat[xc] = flat[xc % 2].T
        r_done = pltpu.make_async_copy(rnat, r_out, ysem)
        r_done.start()
        for q in range(4):
            pltpu.make_async_copy(wst.at[pl.ds(8 * q, 8)], w_out.at[pl.ds(8 * q, 8)], wsem.at[q]).wait()
        r_done.wait()

    return kernel


def solution(mesh):
    samp_size = mesh.shape["samp"]
    design_spec = P(("problem", "samp"), "feat")
    rows_spec = P(("problem", "samp"), None)
    coef_spec = P(("problem", "feat"), None)
    step_spec = P(("problem", "feat"))
    ridge_spec = P("problem")

    def local(design, targets, coef_init, step_sizes, ridge_weights):
        rows, cols = design.shape
        n_tgt = targets.shape[1]
        tgt = n_tgt // STREAMS
        half = tgt // 2
        own = (STREAMS, RING, RING, 2, tgt, 256)
        vm = pltpu.VMEM
        dma = pltpu.SemaphoreType.DMA
        any_spec = pl.BlockSpec(memory_space=pl.ANY)
        vmem_spec = pl.BlockSpec(memory_space=pltpu.VMEM)
        w_t, r_t = pl.pallas_call(
            make_kernel(rows * samp_size, tgt),
            out_shape=(jax.ShapeDtypeStruct((32, 256, n_tgt), F32), jax.ShapeDtypeStruct((rows // LANES, LANES, n_tgt), F32)),
            in_specs=[any_spec, any_spec, any_spec, vmem_spec, vmem_spec],
            out_specs=(any_spec, any_spec),
            scratch_shapes=[
                vm((32, rows, 256), BF16),
                vm((32, 256, LANES), F32),
                vm((LANES, LANES), F32),
                vm((rows // LANES, LANES, n_tgt), F32),
                vm((2, LANES, n_tgt), F32),
                vm(own, BF16),
                vm(own, F32),
                vm((STREAMS, 2, RING, 2, RING, tgt, LANES), F32),
                vm((STREAMS, 2, 2, RING, tgt, LANES), F32),
                vm((STREAMS, 2, 2, RING, tgt, LANES), F32),
                vm((STREAMS, 2, 2, RING, tgt, LANES), F32),
                vm((STREAMS, 2, 3, 2, tgt, LANES), F32),
                vm((STREAMS, 2, 2, tgt, LANES), F32),
                vm((STREAMS, tgt, LANES), F32),
                vm((STREAMS, tgt, rows), BF16),
                vm((STREAMS, tgt, rows), F32),
                vm((STREAMS, FEATS, half, LANES), BF16),
                vm((STREAMS, FEATS, half, LANES), BF16),
                vm((STREAMS, FEATS, half, LANES), BF16),
                vm((STREAMS, half, LANES), F32),
                vm((STREAMS, FEATS, half, LANES), F32),
                dma((32,)),
                dma((4,)),
                dma,
                dma((STREAMS, 2 * AG_MSGS)),
                dma((STREAMS, RS_MSGS)),
                dma((STREAMS, 2 * AG_MSGS)),
                dma((STREAMS, 2 * AG_MSGS)),
                dma((STREAMS, 2 * AG_MSGS)),
                dma((STREAMS, FEATS)),
                dma((STREAMS, FEATS)),
                dma((STREAMS, FEATS)),
                dma((STREAMS, FEATS)),
            ],
            compiler_params=pltpu.CompilerParams(collective_id=0, has_side_effects=True, vmem_limit_bytes=60 * 1024 * 1024),
        )(design, targets, coef_init.reshape(32, 256, n_tgt), step_sizes.reshape(cols // LANES, LANES), ridge_weights.reshape(1, n_tgt))
        coef = w_t.reshape(cols, n_tgt)
        resid = r_t.reshape(rows, n_tgt)
        return coef, resid

    return jax.shard_map(local, mesh=mesh, in_specs=(design_spec, rows_spec, coef_spec, step_spec, ridge_spec), out_specs=(coef_spec, rows_spec), check_vma=False)
```

```python
import jax
import jax.numpy as jnp
from jax import lax
from jax.experimental import pallas as pl
from jax.experimental.pallas import tpu as pltpu
from jax.sharding import PartitionSpec as P

SWEEPS = 4
STEP_WEIGHT = 0.5
RING = 4
FEATS = 8
LANES = 128
ORDER = (2, 1, 3, 0)
STREAMS = 4
MESH_ID = pl.DeviceIdType.MESH
AG_MSGS = 19
RS_MSGS = 26
F32 = jnp.float32
BF16 = jnp.bfloat16


def make_kernel(total_rows, tgt):
    half = tgt // 2
    inv_rows = 1.0 / total_rows

    def kernel(x_hbm, y_hbm, w0_hbm, eta_ref, lam_ref, w_out, r_out,
               xv, wst, yst, rnat, flat, sg, wg, gt, fin, din, cin, r2in, wown, lamb, rt, acc,
               ub, urecv, rbuf, rown, rfin,
               xsem, wsem, ysem, rs_send, rs_recv, ag_recv, w_send, w_recv, x_send, u_recv, r_recv, rf_recv):
        samp = lax.axis_index("samp")
        feat = lax.axis_index("feat")
        zpos = samp // RING
        ypos = samp % RING

        def wrap(v):
            return lax.rem(v + RING, RING)

        def dev(z, y):
            return (0, z * RING + y, feat)

        z_plus, z_minus = dev(wrap(zpos + 1), ypos), dev(wrap(zpos - 1), ypos)
        y_plus, y_minus = dev(zpos, wrap(ypos + 1)), dev(zpos, wrap(ypos - 1))
        first_nbr = ((y_plus, y_minus), (z_plus, z_minus))
        second_nbr = ((z_plus, z_minus), (y_plus, y_minus))

        def place(h, o1, o2):
            if h == 0:
                return wrap(zpos + o2), wrap(ypos + o1)
            return wrap(zpos + o1), wrap(ypos + o2)

        def peer(k):
            return lax.rem(feat + k, FEATS)

        x_copies = [pltpu.make_async_copy(x_hbm.at[:, pl.ds(c * 256, 256)], xv.at[c], xsem.at[c]) for c in range(32)]
        w_copy = pltpu.make_async_copy(w0_hbm.at[pl.ds(samp * 2, 2)], wst.at[pl.ds(0, 2)], wsem.at[0])
        y_copy = pltpu.make_async_copy(y_hbm.at[pl.ds(pl.multiple_of((feat // 2) * LANES, LANES), LANES)], yst, ysem)
        w_copy.start()
        y_copy.start()
        for copy in x_copies:
            copy.start()

        barrier = pltpu.get_barrier_semaphore()
        for nbr in (z_plus, z_minus, y_plus, y_minus, dev(wrap(zpos + 2), ypos), dev(zpos, wrap(ypos + 2))):
            pl.semaphore_signal(barrier, inc=1, device_id=nbr, device_id_type=MESH_ID)
        for k in range(1, FEATS):
            pl.semaphore_signal(barrier, inc=1, device_id=(0, samp, peer(k)), device_id_type=MESH_ID)
        pl.semaphore_wait(barrier, 6 + FEATS - 1)

        def remote(src, dst, send, recv, to):
            return pltpu.make_async_remote_copy(src_ref=src, dst_ref=dst, send_sem=send, recv_sem=recv, device_id=to, device_id_type=MESH_ID)

        def rs1(t, h, kind, way, part):
            io, pm = {"F": (2, way), "D": (1 + 2 * way, 1 - way), "C": (1 + 2 * way, way)}[kind]
            land = {"F": fin, "D": din, "C": cin}[kind]
            rows = pl.ds(0, 4) if kind == "D" else pl.ds(2 * part, 2)
            slot = (h * 2 + way) * 5 + {"F": part, "C": 2 + part, "D": 4}[kind]
            return remote(gt.at[t, h, io, pm, rows], land.at[t, h, way, rows], rs_send.at[t, slot], rs_recv.at[t, slot], first_nbr[h][way])

        def rs2(t, h, js):
            jo = ORDER[js]
            slot = 20 + h * 3 + js
            zi, yi = place(h, 0, jo)
            return remote(gt.at[t, h, 0, :, js], r2in.at[t, h, js], rs_send.at[t, slot], rs_recv.at[t, slot], dev(zi, yi))

        def ag(t, h, idx, buf, send, recv):
            if idx < 3:
                (o1, o2), rows = (0, 0), None
                to = dev(*place(h, 0, ORDER[idx]))
            elif idx < 11:
                way, m = (idx - 3) // 4, (idx - 3) % 4
                to, o1, rows = first_nbr[h][way], 0, None
                o2 = (0, -1, 1, 2)[m]
            else:
                way, m = (idx - 11) // 4, (idx - 11) % 4
                to, o1, rows = first_nbr[h][way], (-1, 1)[way], way
                o2 = (0, -1, 1, 2)[m]
            zi, yi = place(h, o1, o2)
            ref = buf.at[t, zi, yi, h] if rows is None else buf.at[t, zi, yi, h, pl.ds(rows * half, half)]
            slot = h * AG_MSGS + idx
            return remote(ref, ref, send.at[t, slot], recv.at[t, slot], to)

        def go(t, h, net, *idxs):
            for idx in idxs:
                ag(t, h, idx, *net).start()

        def got(t, h, net, *idxs):
            for idx in idxs:
                ag(t, h, idx, *net).wait_recv()

        step_net = (sg, rs_send, ag_recv)
        coef_net = (wg, w_send, w_recv)

        def gather_open(t, net):
            for h in range(2):
                go(t, h, net, 1, 2, 0, 3, 7)

        def gather_second(t, net):
            for h in range(2):
                got(t, h, net, 1)
                go(t, h, net, 4, 8)
                got(t, h, net, 2)
                go(t, h, net, 5, 9)
            for h in range(2):
                got(t, h, net, 0)
                go(t, h, net, 6, 10)
            for h in range(2):
                got(t, h, net, 3)
                go(t, h, net, 11)
                got(t, h, net, 7)
                go(t, h, net, 15)

        def gather_third(t, net):
            for h in range(2):
                for m in range(1, 4):
                    got(t, h, net, 3 + m)
                    go(t, h, net, 11 + m)
                    got(t, h, net, 7 + m)
                    go(t, h, net, 15 + m)

        def gather_close(t, net):
            for h in range(2):
                got(t, h, net, *range(11, 19))
            for h in range(2):
                for idx in range(AG_MSGS):
                    ag(t, h, idx, *net).wait_send()

        def slopes(t, io):
            for h in range(2):
                for js in range(RING):
                    zi, yi = place(h, io, ORDER[js])
                    res = jnp.dot(rt[t], xv[(zi * RING + yi) * 2 + h], preferred_element_type=F32)
                    gt[t, h, io, 0, js] = res[:, :LANES]
                    gt[t, h, io, 1, js] = res[:, LANES:]
                    if io == 2 and js % 2:
                        rs1(t, h, "F", 0, js // 2).start()
                        rs1(t, h, "F", 1, js // 2).start()
                if io % 2:
                    rs1(t, h, "D", io // 2, 0).start()

        def sum_first(t):
            for part in range(2):
                rows = pl.ds(2 * part, 2)
                for h in range(2):
                    for way in range(2):
                        rs1(t, h, "F", way, part).wait_recv()
                        gt[t, h, 1 + 2 * way, way, rows] += fin[t, h, way, rows]
                        rs1(t, h, "C", way, part).start()

        def sum_second(t):
            for part in range(2):
                for h in range(2):
                    for way in range(2):
                        if part == 0:
                            rs1(t, h, "D", way, 0).wait_recv()
                        rs1(t, h, "C", way, part).wait_recv()
                    for js in range(2 * part, 2 * part + 2):
                        for pm in range(2):
                            gt[t, h, 0, pm, js] = gt[t, h, 0, pm, js] + cin[t, h, pm, js] + din[t, h, 1 - pm, js]
                        if js < 3:
                            rs2(t, h, js).start()

        def take_step(t):
            for h in range(2):
                for js in range(3):
                    rs2(t, h, js).wait_recv()
                for pm in range(2):
                    grad = (gt[t, h, 0, pm, 3] + r2in[t, h, 0, pm] + r2in[t, h, 1, pm] + r2in[t, h, 2, pm]) * inv_rows
                    old = wown[t, h, pm]
                    step = eta_ref[pl.ds((samp * 2 + h) * 2 + pm, 1), :] * (grad - lamb[t] * old)
                    wown[t, h, pm] = old + STEP_WEIGHT * step
                    sg[t, zpos, ypos, h, :, pl.ds(pm * LANES, LANES)] = step.astype(BF16)
            for h in range(2):
                for way in range(2):
                    rs1(t, h, "D", way, 0).wait_send()
                    for part in range(2):
                        rs1(t, h, "F", way, part).wait_send()
                        rs1(t, h, "C", way, part).wait_send()
                for js in range(3):
                    rs2(t, h, js).wait_send()

        def coef_open(t):
            for h in range(2):
                for pm in range(2):
                    wg[t, zpos, ypos, h, :, pl.ds(pm * LANES, LANES)] = wown[t, h, pm]
            gather_open(t, coef_net)

        def products(t, o1):
            part = None
            for h in range(2):
                for o2 in (0, -1, 1, 2):
                    zi, yi = place(h, o1, o2)
                    c = (zi * RING + yi) * 2 + h
                    prod = lax.dot_general(sg[t, zi, yi, h], xv[c], (((1,), (1,)), ((), ())), preferred_element_type=F32)
                    part = prod if part is None else part + prod
            acc[t] = part if o1 == 0 else acc[t] + part

        def xmsg(t, k, src, dst, recv):
            return remote(src, dst, x_send.at[t, k], recv.at[t, k], (0, samp, peer(k)))

        def umsg(t, k):
            return xmsg(t, k, ub.at[t, peer(k)], urecv.at[t, feat], u_recv)

        def rmsg(t, k):
            return xmsg(t, k, rbuf.at[t, feat], rbuf.at[t, feat], r_recv)

        def fmsg(t, k):
            return xmsg(t, k, rfin.at[t, feat], rfin.at[t, feat], rf_recv)

        def blocks_out(t):
            for j in range(FEATS):
                ub[t, j] = acc[t, pl.ds((j % 2) * half, half), pl.ds((j // 2) * LANES, LANES)].astype(BF16)
            for k in range(1, FEATS):
                umsg(t, k).start()
            urecv[t, feat] = ub[t, feat]

        def residual(t, weight):
            for k in range(1, FEATS):
                umsg(t, k).wait()
            total = urecv[t, 0].astype(F32)
            for j in range(1, FEATS):
                total = total + urecv[t, j].astype(F32)
            rown[t] = rown[t] - weight * total

        def residual_out(t):
            rbuf[t, feat] = rown[t].astype(BF16)
            for k in range(1, FEATS):
                rmsg(t, k).start()

        def residual_final(t):
            rfin[t, feat] = rown[t]
            for k in range(1, FEATS):
                fmsg(t, k).start()

        def residual_in(t):
            for k in range(1, FEATS):
                rmsg(t, k).wait()
            for j in range(FEATS):
                rt[t, pl.ds((j % 2) * half, half), pl.ds((j // 2) * LANES, LANES)] = rbuf[t, j]

        lam_cols = jnp.broadcast_to(lam_ref[...], (LANES, LANES)).T
        for t in range(STREAMS):
            lamb[t] = lam_cols[t * tgt:(t + 1) * tgt]
        y_copy.wait()
        y_cols = yst[...].T
        core = lax.rem(feat, 2)
        yst[...] = y_cols
        for t in range(STREAMS):
            rown[t] = yst[pl.ds(pl.multiple_of(t * tgt + core * half, half), half), :]
        w_copy.wait()
        for h in range(2):
            for pm in range(2):
                cols = wst[h, pl.ds(pm * LANES, LANES), :].T
                for t in range(STREAMS):
                    mine = cols[t * tgt:(t + 1) * tgt]
                    wown[t, h, pm] = mine
                    sg[t, zpos, ypos, h, :, pl.ds(pm * LANES, LANES)] = mine.astype(BF16)

        for t in range(STREAMS):
            gather_open(t, step_net)
        for copy in x_copies:
            copy.wait()

        rounds = STREAMS * SWEEPS

        def one_pass(i, carry):
            ta, tb, tc, td = (lax.rem(i + off, STREAMS) for off in (2, 1, 0, 3))
            in_a = (i >= 2) & (i < 2 + rounds)
            in_b = (i >= 3) & (i < 3 + rounds)
            in_c = i < STREAMS + rounds
            in_d = i >= 1
            wrap_up = i >= 3 + rounds - STREAMS
            ending = i >= 1 + rounds
            weight = jnp.where(i <= STREAMS, 1.0, STEP_WEIGHT).astype(F32)

            @pl.when(in_a)
            def _():
                residual_in(ta)
                slopes(ta, 2)

            @pl.when(in_b)
            def _():
                sum_second(tb)

            @pl.when(in_d)
            def _():
                gather_close(td, step_net)
                products(td, 2)
                blocks_out(td)

            @pl.when(in_c)
            def _():
                gather_second(tc, step_net)

            @pl.when(in_a)
            def _():
                slopes(ta, 1)
                slopes(ta, 3)
                slopes(ta, 0)

            @pl.when(in_a)
            def _():
                sum_first(ta)

            @pl.when(in_d)
            def _():
                residual(td, weight)

            @pl.when(in_d & jnp.logical_not(ending))
            def _():
                residual_out(td)

            @pl.when(ending)
            def _():
                residual_final(td)

            @pl.when(in_c)
            def _():
                products(tc, 0)

            @pl.when(in_c)
            def _():
                gather_third(tc, step_net)

            @pl.when(in_b)
            def _():
                take_step(tb)
                gather_open(tb, step_net)

            @pl.when(in_b & wrap_up)
            def _():
                coef_open(tb)

            @pl.when((i > 2 + rounds - STREAMS + 1) & in_c)
            def _():
                gather_second(tc, coef_net)

            @pl.when(i > 2 + rounds - STREAMS + 2)
            def _():
                gather_third(td, coef_net)

            @pl.when(in_c)
            def _():
                products(tc, -1)
                products(tc, 1)

            return carry

        lax.fori_loop(0, rounds + STREAMS + 1, one_pass, 0)

        for t in range(STREAMS):
            gather_close(t, coef_net)
            for k in range(1, FEATS):
                fmsg(t, k).wait()

        for q in range(4):
            def flop(c, carry, q=q):
                for pm in range(2):
                    for t in range(STREAMS):
                        flat[pm, t * tgt:(t + 1) * tgt] = wg[t, q, c // 2, lax.rem(c, 2), :, pl.ds(pm * LANES, LANES)]
                for pm in range(2):
                    wst[8 * q + c, pl.ds(pm * LANES, LANES), :] = flat[pm].T
                return carry

            lax.fori_loop(0, 8, flop, 0)
            pltpu.make_async_copy(wst.at[pl.ds(8 * q, 8)], w_out.at[pl.ds(8 * q, 8)], wsem.at[q]).start()
        for xc in range(4):
            for t in range(STREAMS):
                for core_id in range(2):
                    flat[xc % 2, pl.ds(t * tgt + core_id * half, half), :] = rfin[t, 2 * xc + core_id]
            rnat[xc] = flat[xc % 2].T
        r_done = pltpu.make_async_copy(rnat, r_out, ysem)
        r_done.start()
        for q in range(4):
            pltpu.make_async_copy(wst.at[pl.ds(8 * q, 8)], w_out.at[pl.ds(8 * q, 8)], wsem.at[q]).wait()
        r_done.wait()

    return kernel


def solution(mesh):
    samp_size = mesh.shape["samp"]
    design_spec = P(("problem", "samp"), "feat")
    rows_spec = P(("problem", "samp"), None)
    coef_spec = P(("problem", "feat"), None)
    step_spec = P(("problem", "feat"))
    ridge_spec = P("problem")

    def local(design, targets, coef_init, step_sizes, ridge_weights):
        rows, cols = design.shape
        n_tgt = targets.shape[1]
        tgt = n_tgt // STREAMS
        half = tgt // 2
        own = (STREAMS, RING, RING, 2, tgt, 256)
        vm = pltpu.VMEM
        dma = pltpu.SemaphoreType.DMA
        any_spec = pl.BlockSpec(memory_space=pl.ANY)
        vmem_spec = pl.BlockSpec(memory_space=pltpu.VMEM)
        w_t, r_t = pl.pallas_call(
            make_kernel(rows * samp_size, tgt),
            out_shape=(jax.ShapeDtypeStruct((32, 256, n_tgt), F32), jax.ShapeDtypeStruct((rows // LANES, LANES, n_tgt), F32)),
            in_specs=[any_spec, any_spec, any_spec, vmem_spec, vmem_spec],
            out_specs=(any_spec, any_spec),
            scratch_shapes=[
                vm((32, rows, 256), BF16),
                vm((32, 256, LANES), F32),
                vm((LANES, LANES), F32),
                vm((rows // LANES, LANES, n_tgt), F32),
                vm((2, LANES, n_tgt), F32),
                vm(own, BF16),
                vm(own, F32),
                vm((STREAMS, 2, RING, 2, RING, tgt, LANES), F32),
                vm((STREAMS, 2, 2, RING, tgt, LANES), F32),
                vm((STREAMS, 2, 2, RING, tgt, LANES), F32),
                vm((STREAMS, 2, 2, RING, tgt, LANES), F32),
                vm((STREAMS, 2, 3, 2, tgt, LANES), F32),
                vm((STREAMS, 2, 2, tgt, LANES), F32),
                vm((STREAMS, tgt, LANES), F32),
                vm((STREAMS, tgt, rows), BF16),
                vm((STREAMS, tgt, rows), F32),
                vm((STREAMS, FEATS, half, LANES), BF16),
                vm((STREAMS, FEATS, half, LANES), BF16),
                vm((STREAMS, FEATS, half, LANES), BF16),
                vm((STREAMS, half, LANES), F32),
                vm((STREAMS, FEATS, half, LANES), F32),
                dma((32,)),
                dma((4,)),
                dma,
                dma((STREAMS, 2 * AG_MSGS)),
                dma((STREAMS, RS_MSGS)),
                dma((STREAMS, 2 * AG_MSGS)),
                dma((STREAMS, 2 * AG_MSGS)),
                dma((STREAMS, 2 * AG_MSGS)),
                dma((STREAMS, FEATS)),
                dma((STREAMS, FEATS)),
                dma((STREAMS, FEATS)),
                dma((STREAMS, FEATS)),
            ],
            compiler_params=pltpu.CompilerParams(collective_id=0, has_side_effects=True, vmem_limit_bytes=60 * 1024 * 1024),
        )(design, targets, coef_init.reshape(32, 256, n_tgt), step_sizes.reshape(cols // LANES, LANES), ridge_weights.reshape(1, n_tgt))
        coef = w_t.reshape(cols, n_tgt)
        resid = r_t.reshape(rows, n_tgt)
        return coef, resid

    return jax.shard_map(local, mesh=mesh, in_specs=(design_spec, rows_spec, coef_spec, step_spec, ridge_spec), out_specs=(coef_spec, rows_spec), check_vma=False)
```

```python
import jax
import jax.numpy as jnp
from jax import lax
from jax.experimental import pallas as pl
from jax.experimental.pallas import tpu as pltpu
from jax.sharding import PartitionSpec as P

SWEEPS = 4
STEP_WEIGHT = 0.5
RING = 4
FEATS = 8
LANES = 128
ORDER = (2, 1, 3, 0)
STREAMS = 4
MESH_ID = pl.DeviceIdType.MESH
AG_MSGS = 19
RS_MSGS = 26
F32 = jnp.float32
BF16 = jnp.bfloat16


def flip_results(w_ref, r_ref, coef_ref, resid_ref):
    for y in range(2):
        for h in range(2):
            for pm in range(2):
                cols = [w_ref[t, 0, y, h, :, pl.ds(pm * LANES, LANES)] for t in range(STREAMS)]
                coef_ref[pl.ds(((y * 2 + h) * 2 + pm) * LANES, LANES), :] = jnp.concatenate(cols, axis=0).T

    @pl.when(pl.program_id(0) == 0)
    def _():
        for xq in range(4):
            cols = [r_ref[t, 2 * xq + side] for t in range(STREAMS) for side in range(2)]
            resid_ref[pl.ds(xq * LANES, LANES), :] = jnp.concatenate(cols, axis=0).T


def make_kernel(total_rows, tgt):
    half = tgt // 2
    inv_rows = 1.0 / total_rows

    def kernel(x_hbm, y_hbm, w0_hbm, eta_ref, lam_ref, w_out, r_out,
               xv, xt, wst, yst, uacc, sg, wg, gt, fin, din, cin, r2in, wown, lamb, rt, acc,
               ub, urecv, rbuf, rown, rfin,
               xsem, wsem, ysem, rs_send, rs_recv, ag_recv, w_send, w_recv, x_send, u_recv, r_recv, rf_recv):
        samp = lax.axis_index("samp")
        feat = lax.axis_index("feat")
        zpos = samp // RING
        ypos = samp % RING

        def wrap(v):
            return lax.rem(v + RING, RING)

        def dev(z, y):
            return (0, z * RING + y, feat)

        z_plus, z_minus = dev(wrap(zpos + 1), ypos), dev(wrap(zpos - 1), ypos)
        y_plus, y_minus = dev(zpos, wrap(ypos + 1)), dev(zpos, wrap(ypos - 1))
        first_nbr = ((y_plus, y_minus), (z_plus, z_minus))
        second_nbr = ((z_plus, z_minus), (y_plus, y_minus))

        def place(h, o1, o2):
            if h == 0:
                return wrap(zpos + o2), wrap(ypos + o1)
            return wrap(zpos + o1), wrap(ypos + o2)

        def peer(k):
            return lax.rem(feat + k, FEATS)

        x_copies = [pltpu.make_async_copy(x_hbm.at[:, pl.ds(c * 256, 256)], xv.at[c], xsem.at[c]) for c in range(32)]
        w_copies = [pltpu.make_async_copy(w0_hbm.at[pl.ds(8 * q, 8)], wst.at[pl.ds(8 * q, 8)], wsem.at[q]) for q in range(4)]
        y_copy = pltpu.make_async_copy(y_hbm.at[pl.ds(pl.multiple_of((feat // 2) * LANES, LANES), LANES)], yst, ysem)
        y_copy.start()
        for q in range(4):
            w_copies[q].start()
            for c in range(8 * q, 8 * q + 8):
                x_copies[c].start()

        barrier = pltpu.get_barrier_semaphore()
        for nbr in (z_plus, z_minus, y_plus, y_minus, dev(wrap(zpos + 2), ypos), dev(zpos, wrap(ypos + 2))):
            pl.semaphore_signal(barrier, inc=1, device_id=nbr, device_id_type=MESH_ID)
        for k in range(1, FEATS):
            pl.semaphore_signal(barrier, inc=1, device_id=(0, samp, peer(k)), device_id_type=MESH_ID)
        pl.semaphore_wait(barrier, 6 + FEATS - 1)

        def remote(src, dst, send, recv, to):
            return pltpu.make_async_remote_copy(src_ref=src, dst_ref=dst, send_sem=send, recv_sem=recv, device_id=to, device_id_type=MESH_ID)

        def rs1(t, h, kind, way, part):
            io, pm = {"F": (2, way), "D": (1 + 2 * way, 1 - way), "C": (1 + 2 * way, way)}[kind]
            land = {"F": fin, "D": din, "C": cin}[kind]
            rows = pl.ds(0, 4) if kind == "D" else pl.ds(2 * part, 2)
            slot = (h * 2 + way) * 5 + {"F": part, "C": 2 + part, "D": 4}[kind]
            return remote(gt.at[t, h, io, pm, rows], land.at[t, h, way, rows], rs_send.at[t, slot], rs_recv.at[t, slot], first_nbr[h][way])

        def rs2(t, h, js):
            jo = ORDER[js]
            slot = 20 + h * 3 + js
            zi, yi = place(h, 0, jo)
            return remote(gt.at[t, h, 0, :, js], r2in.at[t, h, js], rs_send.at[t, slot], rs_recv.at[t, slot], dev(zi, yi))

        def ag(t, h, idx, buf, send, recv):
            if idx < 3:
                (o1, o2), rows = (0, 0), None
                to = dev(*place(h, 0, ORDER[idx]))
            elif idx < 11:
                way, m = (idx - 3) // 4, (idx - 3) % 4
                to, o1, rows = first_nbr[h][way], 0, None
                o2 = (0, -1, 1, 2)[m]
            else:
                way, m = (idx - 11) // 4, (idx - 11) % 4
                to, o1, rows = first_nbr[h][way], (-1, 1)[way], way
                o2 = (0, -1, 1, 2)[m]
            zi, yi = place(h, o1, o2)
            ref = buf.at[t, zi, yi, h] if rows is None else buf.at[t, zi, yi, h, pl.ds(rows * half, half)]
            slot = h * AG_MSGS + idx
            return remote(ref, ref, send.at[t, slot], recv.at[t, slot], to)

        def go(t, h, net, *idxs):
            for idx in idxs:
                ag(t, h, idx, *net).start()

        def got(t, h, net, *idxs):
            for idx in idxs:
                ag(t, h, idx, *net).wait_recv()

        step_net = (sg, rs_send, ag_recv)
        coef_net = (wg, w_send, w_recv)

        def gather_open(t, net):
            for h in range(2):
                go(t, h, net, 1, 2, 0, 3, 7)

        def gather_second(t, net):
            for h in range(2):
                got(t, h, net, 1)
                go(t, h, net, 4, 8)
                got(t, h, net, 2)
                go(t, h, net, 5, 9)
            for h in range(2):
                got(t, h, net, 0)
                go(t, h, net, 6, 10)
            for h in range(2):
                got(t, h, net, 3)
                go(t, h, net, 11)
                got(t, h, net, 7)
                go(t, h, net, 15)

        def gather_third(t, net):
            for h in range(2):
                for m in range(1, 4):
                    got(t, h, net, 3 + m)
                    go(t, h, net, 11 + m)
                    got(t, h, net, 7 + m)
                    go(t, h, net, 15 + m)

        def gather_close(t, net):
            for h in range(2):
                got(t, h, net, *range(11, 19))
            for h in range(2):
                for idx in range(AG_MSGS):
                    ag(t, h, idx, *net).wait_send()

        def slopes(t, *ios):
            for io in ios:
                for h in range(2):
                    for js in range(RING):
                        zi, yi = place(h, io, ORDER[js])
                        res = jnp.dot(rt[t], xv[(zi * RING + yi) * 2 + h], preferred_element_type=F32)
                        gt[t, h, io, 0, js] = res[:, :LANES]
                        gt[t, h, io, 1, js] = res[:, LANES:]
            for io in ios:
                for h in range(2):
                    if io == 2:
                        for part in range(2):
                            rs1(t, h, "F", 0, part).start()
                            rs1(t, h, "F", 1, part).start()
                    elif io:
                        rs1(t, h, "D", io // 2, 0).start()

        def sum_first(t):
            for part in range(2):
                rows = pl.ds(2 * part, 2)
                for h in range(2):
                    for way in range(2):
                        rs1(t, h, "F", way, part).wait_recv()
                        gt[t, h, 1 + 2 * way, way, rows] += fin[t, h, way, rows]
                        rs1(t, h, "C", way, part).start()

        def sum_second(t):
            for part in range(2):
                for h in range(2):
                    for way in range(2):
                        if part == 0:
                            rs1(t, h, "D", way, 0).wait_recv()
                        rs1(t, h, "C", way, part).wait_recv()
                    for js in range(2 * part, 2 * part + 2):
                        for pm in range(2):
                            gt[t, h, 0, pm, js] = gt[t, h, 0, pm, js] + cin[t, h, pm, js] + din[t, h, 1 - pm, js]
                        if js < 3:
                            rs2(t, h, js).start()

        def take_step(t):
            for h in range(2):
                for js in range(3):
                    rs2(t, h, js).wait_recv()
                for pm in range(2):
                    grad = (gt[t, h, 0, pm, 3] + r2in[t, h, 0, pm] + r2in[t, h, 1, pm] + r2in[t, h, 2, pm]) * inv_rows
                    old = wown[t, h, pm]
                    step = eta_ref[pl.ds((samp * 2 + h) * 2 + pm, 1), :] * (grad - lamb[t] * old)
                    wown[t, h, pm] = old + STEP_WEIGHT * step
                    sg[t, zpos, ypos, h, :, pl.ds(pm * LANES, LANES)] = step.astype(BF16)
            for h in range(2):
                for way in range(2):
                    rs1(t, h, "D", way, 0).wait_send()
                    for part in range(2):
                        rs1(t, h, "F", way, part).wait_send()
                        rs1(t, h, "C", way, part).wait_send()
                for js in range(3):
                    rs2(t, h, js).wait_send()

        def coef_open(t):
            for h in range(2):
                for pm in range(2):
                    wg[t, zpos, ypos, h, :, pl.ds(pm * LANES, LANES)] = wown[t, h, pm]
            gather_open(t, coef_net)

        def products(t, o1):
            part = None
            for h in range(2):
                for o2 in (0, -1, 1, 2):
                    zi, yi = place(h, o1, o2)
                    c = (zi * RING + yi) * 2 + h
                    prod = jnp.dot(sg[t, zi, yi, h], xt[c], preferred_element_type=F32)
                    part = prod if part is None else part + prod
            acc[t] = part if o1 == 0 else acc[t] + part

        def xmsg(t, k, src, dst, recv):
            return remote(src, dst, x_send.at[t, k], recv.at[t, k], (0, samp, peer(k)))

        def umsg(t, k):
            return xmsg(t, k, ub.at[t, peer(k)], urecv.at[t, feat], u_recv)

        def rmsg(t, k):
            return xmsg(t, k, rbuf.at[t, feat], rbuf.at[t, feat], r_recv)

        def fmsg(t, k):
            return xmsg(t, k, rfin.at[t, feat], rfin.at[t, feat], rf_recv)

        def blocks_out(t):
            for j in range(FEATS):
                ub[t, j] = acc[t, pl.ds((j % 2) * half, half), pl.ds((j // 2) * LANES, LANES)].astype(BF16)
            blocks_send(t)

        def blocks_send(t):
            for k in range(1, FEATS):
                umsg(t, k).start()
            urecv[t, feat] = ub[t, feat]

        def residual(t, weight):
            for k in range(1, FEATS):
                umsg(t, k).wait()
            total = urecv[t, 0].astype(F32)
            for j in range(1, FEATS):
                total = total + urecv[t, j].astype(F32)
            rown[t] = rown[t] - weight * total

        def residual_out(t):
            rbuf[t, feat] = rown[t].astype(BF16)
            for k in range(1, FEATS):
                rmsg(t, k).start()

        def residual_final(t):
            rfin[t, feat] = rown[t]
            for k in range(1, FEATS):
                fmsg(t, k).start()

        def residual_in(t):
            for k in range(1, FEATS):
                rmsg(t, k).wait()
            for j in range(FEATS):
                rt[t, pl.ds((j % 2) * half, half), pl.ds((j // 2) * LANES, LANES)] = rbuf[t, j]

        lam_cols = jnp.broadcast_to(lam_ref[...], (LANES, LANES)).T
        for t in range(STREAMS):
            lamb[t] = lam_cols[t * tgt:(t + 1) * tgt]
        y_copy.wait()
        y_cols = yst[...].T
        core = lax.rem(feat, 2)
        yst[...] = y_cols
        for t in range(STREAMS):
            rown[t] = yst[pl.ds(pl.multiple_of(t * tgt + core * half, half), half), :]
        for q in range(4):
            w_copies[q].wait()
            for c in range(8 * q, 8 * q + 8):
                x_copies[c].wait()

            def start_block(g, carry, q=q):
                part = None
                for j in range(4):
                    c = 8 * q + 4 * g + j
                    prod = jnp.dot(xv[c], wst[c].astype(BF16), preferred_element_type=F32)
                    part = prod if part is None else part + prod
                uacc[...] = uacc[...] + part
                return carry

            if q == 0:
                uacc[...] = jnp.zeros_like(uacc)
            lax.fori_loop(0, 2, start_block, 0)
        for xq in range(4):
            cols = uacc[pl.ds(xq * LANES, LANES), :].T
            for t in range(STREAMS):
                for side in range(2):
                    row = t * tgt + side * half
                    ub[t, 2 * xq + side] = cols[row:row + half].astype(BF16)
        for t in range(STREAMS):
            blocks_send(t)
        for h in range(2):
            for pm in range(2):
                cols = wst[samp * 2 + h, pl.ds(pm * LANES, LANES), :].T
                for t in range(STREAMS):
                    wown[t, h, pm] = cols[t * tgt:(t + 1) * tgt]

        def turn(c, carry):
            xt[c] = xv[c].T
            return carry

        lax.fori_loop(0, 20, turn, 0)
        for t in range(STREAMS):
            residual(t, 1.0)
            residual_out(t)
        lax.fori_loop(20, 32, turn, 0)

        rounds = STREAMS * SWEEPS

        def one_pass(i, carry):
            ta, tb, tc, td = (lax.rem(i + off, STREAMS) for off in (2, 1, 0, 3))
            in_a = (i >= 2) & (i < 2 + rounds)
            in_b = (i >= 3) & (i < 3 + rounds)
            in_c = (i >= STREAMS) & (i < STREAMS + rounds)
            in_d = i >= 1 + STREAMS
            wrap_up = i >= 3 + rounds - STREAMS
            ending = i >= 1 + rounds

            @pl.when(in_a)
            def _():
                residual_in(ta)
                slopes(ta, 2)

            @pl.when(in_b)
            def _():
                sum_second(tb)

            @pl.when(in_d)
            def _():
                gather_close(td, step_net)
                products(td, 2)
                blocks_out(td)

            @pl.when(in_c)
            def _():
                gather_second(tc, step_net)

            @pl.when(i > 2 + rounds - STREAMS + 2)
            def _():
                gather_third(td, coef_net)

            @pl.when((i > 2 + rounds - STREAMS + 1) & in_c)
            def _():
                gather_second(tc, coef_net)

            @pl.when(in_a)
            def _():
                slopes(ta, 1, 3, 0)

            @pl.when(in_a)
            def _():
                sum_first(ta)

            @pl.when(in_d)
            def _():
                residual(td, STEP_WEIGHT)

            @pl.when(in_d & jnp.logical_not(ending))
            def _():
                residual_out(td)

            @pl.when(ending)
            def _():
                residual_final(td)

            @pl.when(in_c)
            def _():
                products(tc, 0)

            @pl.when(in_c)
            def _():
                gather_third(tc, step_net)

            @pl.when(in_b)
            def _():
                take_step(tb)
                gather_open(tb, step_net)

            @pl.when(in_b & wrap_up)
            def _():
                coef_open(tb)

            @pl.when(in_c)
            def _():
                products(tc, -1)
                products(tc, 1)

            return carry

        lax.fori_loop(2, rounds + STREAMS + 1, one_pass, 0)

        w_done = [pltpu.make_async_copy(wg.at[t], w_out.at[t], wsem.at[t]) for t in range(STREAMS)]
        for t in range(STREAMS):
            for k in range(1, FEATS):
                fmsg(t, k).wait()
        r_done = pltpu.make_async_copy(rfin, r_out, ysem)
        r_done.start()
        for t in range(STREAMS):
            gather_close(t, coef_net)
            w_done[t].start()
        for t in range(STREAMS):
            w_done[t].wait()
        r_done.wait()

    return kernel


def solution(mesh):
    samp_size = mesh.shape["samp"]
    design_spec = P(("problem", "samp"), "feat")
    rows_spec = P(("problem", "samp"), None)
    coef_spec = P(("problem", "feat"), None)
    step_spec = P(("problem", "feat"))
    ridge_spec = P("problem")

    def local(design, targets, coef_init, step_sizes, ridge_weights):
        rows, cols = design.shape
        n_tgt = targets.shape[1]
        tgt = n_tgt // STREAMS
        half = tgt // 2
        own = (STREAMS, RING, RING, 2, tgt, 256)
        vm = pltpu.VMEM
        dma = pltpu.SemaphoreType.DMA
        any_spec = pl.BlockSpec(memory_space=pl.ANY)
        vmem_spec = pl.BlockSpec(memory_space=pltpu.VMEM)
        w_t, r_t = pl.pallas_call(
            make_kernel(rows * samp_size, tgt),
            out_shape=(jax.ShapeDtypeStruct(own, F32), jax.ShapeDtypeStruct((STREAMS, FEATS, half, LANES), F32)),
            in_specs=[any_spec, any_spec, any_spec, vmem_spec, vmem_spec],
            out_specs=(any_spec, any_spec),
            scratch_shapes=[
                vm((32, rows, 256), BF16),
                vm((32, 256, rows), BF16),
                vm((32, 256, LANES), F32),
                vm((LANES, LANES), F32),
                vm((rows, n_tgt), F32),
                vm(own, BF16),
                vm(own, F32),
                vm((STREAMS, 2, RING, 2, RING, tgt, LANES), F32),
                vm((STREAMS, 2, 2, RING, tgt, LANES), F32),
                vm((STREAMS, 2, 2, RING, tgt, LANES), F32),
                vm((STREAMS, 2, 2, RING, tgt, LANES), F32),
                vm((STREAMS, 2, 3, 2, tgt, LANES), F32),
                vm((STREAMS, 2, 2, tgt, LANES), F32),
                vm((STREAMS, tgt, LANES), F32),
                vm((STREAMS, tgt, rows), BF16),
                vm((STREAMS, tgt, rows), F32),
                vm((STREAMS, FEATS, half, LANES), BF16),
                vm((STREAMS, FEATS, half, LANES), BF16),
                vm((STREAMS, FEATS, half, LANES), BF16),
                vm((STREAMS, half, LANES), F32),
                vm((STREAMS, FEATS, half, LANES), F32),
                dma((32,)),
                dma((4,)),
                dma,
                dma((STREAMS, 2 * AG_MSGS)),
                dma((STREAMS, RS_MSGS)),
                dma((STREAMS, 2 * AG_MSGS)),
                dma((STREAMS, 2 * AG_MSGS)),
                dma((STREAMS, 2 * AG_MSGS)),
                dma((STREAMS, FEATS)),
                dma((STREAMS, FEATS)),
                dma((STREAMS, FEATS)),
                dma((STREAMS, FEATS)),
            ],
            compiler_params=pltpu.CompilerParams(collective_id=0, has_side_effects=True, vmem_limit_bytes=60 * 1024 * 1024),
        )(design, targets, coef_init.reshape(32, 256, n_tgt), step_sizes.reshape(cols // LANES, LANES), ridge_weights.reshape(1, n_tgt))
        coef, resid = pl.pallas_call(
            flip_results,
            grid=(8,),
            in_specs=[
                pl.BlockSpec((STREAMS, 1, 2, 2, tgt, 256), lambda g: (0, g // 2, g % 2, 0, 0, 0)),
                pl.BlockSpec((STREAMS, FEATS, half, LANES), lambda g: (0, 0, 0, 0)),
            ],
            out_specs=(pl.BlockSpec((cols // 8, n_tgt), lambda g: (g, 0)), pl.BlockSpec((rows, n_tgt), lambda g: (0, 0))),
            out_shape=(jax.ShapeDtypeStruct((cols, n_tgt), F32), jax.ShapeDtypeStruct((rows, n_tgt), F32)),
        )(w_t, r_t)
        return coef, resid

    return jax.shard_map(local, mesh=mesh, in_specs=(design_spec, rows_spec, coef_spec, step_spec, ridge_spec), out_specs=(coef_spec, rows_spec), check_vma=False)
```

```python
import jax
import jax.numpy as jnp
from jax import lax
from jax.experimental import pallas as pl
from jax.experimental.pallas import tpu as pltpu
from jax.sharding import PartitionSpec as P

SWEEPS = 4
STEP_WEIGHT = 0.5
RING = 4
FEATS = 8
LANES = 128
ORDER = (2, 1, 3, 0)
STREAMS = 4
MESH_ID = pl.DeviceIdType.MESH
AG_MSGS = 19
RS_MSGS = 26
F32 = jnp.float32
BF16 = jnp.bfloat16


def flip_results(w_hbm, r_hbm, coef_hbm, resid_hbm, w_in, r_in, coef, resid, in_sem, out_sem, r_sem):
    loads = [pltpu.make_async_copy(w_hbm.at[:, p // 2, pl.ds(p % 2 * 2, 2)], w_in.at[p], in_sem.at[p]) for p in range(8)]
    stores = [pltpu.make_async_copy(coef.at[p], coef_hbm.at[pl.ds(p * 1024, 1024)], out_sem.at[p]) for p in range(8)]
    r_load = pltpu.make_async_copy(r_hbm, r_in, r_sem.at[0])
    r_store = pltpu.make_async_copy(resid, resid_hbm, r_sem.at[1])
    r_load.start()
    for load in loads:
        load.start()
    r_load.wait()
    for xq in range(4):
        cols = [r_in[t, :, pl.ds(xq * LANES, LANES)] for t in range(STREAMS)]
        resid[pl.ds(xq * LANES, LANES), :] = jnp.concatenate(cols, axis=0).T
    r_store.start()
    for p in range(8):
        loads[p].wait()
        for y in range(2):
            for h in range(2):
                cols = [w_in[p, t, y, h] for t in range(STREAMS)]
                coef[p, pl.ds((y * 2 + h) * 256, 256), :] = jnp.concatenate(cols, axis=0).T
        stores[p].start()
    for p in range(8):
        stores[p].wait()
    r_store.wait()


def make_kernel(total_rows, tgt):
    half = tgt // 2
    inv_rows = 1.0 / total_rows

    def kernel(x_hbm, y_hbm, w0_hbm, eta_hbm, lam_hbm, w_out, r_out,
               eta_ref, lam_ref, xv, xt, wst, yst, uacc, sg, wg, gt, fin, din, cin, r2in, wown, lamb, rt, acc,
               ub, urecv, rown,
               xsem, wsem, psem, ysem, rs_send, rs_recv, ag_recv, w_send, w_recv, x_send, u_recv):
        samp = lax.axis_index("samp")
        feat = lax.axis_index("feat")
        zpos = samp // RING
        ypos = samp % RING

        def wrap(v):
            return lax.rem(v + RING, RING)

        def dev(z, y):
            return (0, z * RING + y, feat)

        z_plus, z_minus = dev(wrap(zpos + 1), ypos), dev(wrap(zpos - 1), ypos)
        y_plus, y_minus = dev(zpos, wrap(ypos + 1)), dev(zpos, wrap(ypos - 1))
        first_nbr = ((y_plus, y_minus), (z_plus, z_minus))
        second_nbr = ((z_plus, z_minus), (y_plus, y_minus))

        def place(h, o1, o2):
            if h == 0:
                return wrap(zpos + o2), wrap(ypos + o1)
            return wrap(zpos + o1), wrap(ypos + o2)

        def peer(k):
            return lax.rem(feat + k, FEATS)

        x_copies = [pltpu.make_async_copy(x_hbm.at[:, pl.ds(c * 256, 256)], xv.at[c], xsem.at[c]) for c in range(32)]
        w_copies = [pltpu.make_async_copy(w0_hbm.at[pl.ds(8 * q, 8)], wst.at[pl.ds(8 * q, 8)], wsem.at[q]) for q in range(4)]
        y_copy = pltpu.make_async_copy(y_hbm, yst, ysem)
        eta_copy = pltpu.make_async_copy(eta_hbm, eta_ref, psem.at[0])
        lam_copy = pltpu.make_async_copy(lam_hbm, lam_ref, psem.at[1])
        for q in range(4):
            w_copies[q].start()
            for c in range(8 * q, 8 * q + 8):
                x_copies[c].start()

        y_copy.start()
        eta_copy.start()
        lam_copy.start()

        barrier = pltpu.get_barrier_semaphore()
        for nbr in (z_plus, z_minus, y_plus, y_minus, dev(wrap(zpos + 2), ypos), dev(zpos, wrap(ypos + 2))):
            pl.semaphore_signal(barrier, inc=1, device_id=nbr, device_id_type=MESH_ID)
        for k in range(1, FEATS):
            pl.semaphore_signal(barrier, inc=1, device_id=(0, samp, peer(k)), device_id_type=MESH_ID)

        def remote(src, dst, send, recv, to):
            return pltpu.make_async_remote_copy(src_ref=src, dst_ref=dst, send_sem=send, recv_sem=recv, device_id=to, device_id_type=MESH_ID)

        def rs1(t, h, kind, way, part):
            io, pm = {"F": (2, way), "D": (1 + 2 * way, 1 - way), "C": (1 + 2 * way, way)}[kind]
            land = {"F": fin, "D": din, "C": cin}[kind]
            rows = pl.ds(0, 4) if kind == "D" else pl.ds(2 * part, 2)
            slot = (h * 2 + way) * 5 + {"F": part, "C": 2 + part, "D": 4}[kind]
            return remote(gt.at[t, h, io, pm, rows], land.at[t, h, way, rows], rs_send.at[t, slot], rs_recv.at[t, slot], first_nbr[h][way])

        def rs2(t, h, js):
            jo = ORDER[js]
            slot = 20 + h * 3 + js
            zi, yi = place(h, 0, jo)
            return remote(gt.at[t, h, 0, :, js], r2in.at[t, h, js], rs_send.at[t, slot], rs_recv.at[t, slot], dev(zi, yi))

        def ag(t, h, idx, buf, send, recv):
            if idx < 3:
                (o1, o2), rows = (0, 0), None
                to = dev(*place(h, 0, ORDER[idx]))
            elif idx < 11:
                way, m = (idx - 3) // 4, (idx - 3) % 4
                to, o1, rows = first_nbr[h][way], 0, None
                o2 = (0, -1, 1, 2)[m]
            else:
                way, m = (idx - 11) // 4, (idx - 11) % 4
                to, o1, rows = first_nbr[h][way], (-1, 1)[way], way
                o2 = (0, -1, 1, 2)[m]
            zi, yi = place(h, o1, o2)
            ref = buf.at[t, zi, yi, h] if rows is None else buf.at[t, zi, yi, h, pl.ds(rows * half, half)]
            slot = h * AG_MSGS + idx
            return remote(ref, ref, send.at[t, slot], recv.at[t, slot], to)

        def go(t, h, net, *idxs):
            for idx in idxs:
                ag(t, h, idx, *net).start()

        def got(t, h, net, *idxs):
            for idx in idxs:
                ag(t, h, idx, *net).wait_recv()

        step_net = (sg, rs_send, ag_recv)
        coef_net = (wg, w_send, w_recv)

        def gather_open(t, net):
            for h in range(2):
                go(t, h, net, 1, 2, 0, 3, 7)

        def gather_second(t, net):
            for h in range(2):
                got(t, h, net, 1)
                go(t, h, net, 4, 8)
                got(t, h, net, 2)
                go(t, h, net, 5, 9)
            for h in range(2):
                got(t, h, net, 0)
                go(t, h, net, 6, 10)
            for h in range(2):
                got(t, h, net, 3)
                go(t, h, net, 11)
                got(t, h, net, 7)
                go(t, h, net, 15)

        def gather_third(t, net):
            for h in range(2):
                for m in range(1, 4):
                    got(t, h, net, 3 + m)
                    go(t, h, net, 11 + m)
                    got(t, h, net, 7 + m)
                    go(t, h, net, 15 + m)

        def gather_close(t, net):
            for h in range(2):
                got(t, h, net, *range(11, 19))
            for h in range(2):
                for idx in range(AG_MSGS):
                    ag(t, h, idx, *net).wait_send()

        def slopes(t, *ios):
            for io in ios:
                for h in range(2):
                    for js in range(RING):
                        zi, yi = place(h, io, ORDER[js])
                        res = jnp.dot(rt[t], xv[(zi * RING + yi) * 2 + h], preferred_element_type=F32)
                        gt[t, h, io, 0, js] = res[:, :LANES]
                        gt[t, h, io, 1, js] = res[:, LANES:]
            for io in ios:
                for h in range(2):
                    if io == 2:
                        for part in range(2):
                            rs1(t, h, "F", 0, part).start()
                            rs1(t, h, "F", 1, part).start()
                    elif io:
                        rs1(t, h, "D", io // 2, 0).start()

        def sum_first(t):
            for part in range(2):
                rows = pl.ds(2 * part, 2)
                for h in range(2):
                    for way in range(2):
                        rs1(t, h, "F", way, part).wait_recv()
                        gt[t, h, 1 + 2 * way, way, rows] += fin[t, h, way, rows]
                        rs1(t, h, "C", way, part).start()

        def sum_second(t):
            for part in range(2):
                for h in range(2):
                    for way in range(2):
                        if part == 0:
                            rs1(t, h, "D", way, 0).wait_recv()
                        rs1(t, h, "C", way, part).wait_recv()
                    for js in range(2 * part, 2 * part + 2):
                        for pm in range(2):
                            gt[t, h, 0, pm, js] = gt[t, h, 0, pm, js] + cin[t, h, pm, js] + din[t, h, 1 - pm, js]
                        if js < 3:
                            rs2(t, h, js).start()

        def take_step(t):
            for h in range(2):
                for js in range(3):
                    rs2(t, h, js).wait_recv()
                for pm in range(2):
                    grad = (gt[t, h, 0, pm, 3] + r2in[t, h, 0, pm] + r2in[t, h, 1, pm] + r2in[t, h, 2, pm]) * inv_rows
                    old = wown[t, h, pm]
                    step = eta_ref[pl.ds((samp * 2 + h) * 2 + pm, 1), :] * (grad - lamb[t] * old)
                    wown[t, h, pm] = old + STEP_WEIGHT * step
                    sg[t, zpos, ypos, h, :, pl.ds(pm * LANES, LANES)] = step.astype(BF16)
            for h in range(2):
                for way in range(2):
                    rs1(t, h, "D", way, 0).wait_send()
                    for part in range(2):
                        rs1(t, h, "F", way, part).wait_send()
                        rs1(t, h, "C", way, part).wait_send()
                for js in range(3):
                    rs2(t, h, js).wait_send()

        def coef_open(t):
            for h in range(2):
                for pm in range(2):
                    wg[t, zpos, ypos, h, :, pl.ds(pm * LANES, LANES)] = wown[t, h, pm]
            gather_open(t, coef_net)

        def products(t, o1):
            part = None
            for h in range(2):
                for o2 in (0, -1, 1, 2):
                    zi, yi = place(h, o1, o2)
                    c = (zi * RING + yi) * 2 + h
                    prod = jnp.dot(sg[t, zi, yi, h], xt[c], preferred_element_type=F32)
                    part = prod if part is None else part + prod
            acc[t] = part if o1 == 0 else acc[t] + part

        def umsg(t, k, side):
            return remote(ub.at[t], urecv.at[side, t, feat], x_send.at[t, k], u_recv.at[side, t, k], (0, samp, peer(k)))

        def blocks_send(t, side):
            for k in range(1, FEATS):
                umsg(t, k, side).start()
            urecv[side, t, feat] = ub[t]

        def blocks_out(t, side):
            ub[t] = acc[t].astype(BF16)
            blocks_send(t, side)

        def residual(t, side, weight):
            for k in range(1, FEATS):
                umsg(t, k, side).wait()
            total = urecv[side, t, 0].astype(F32)
            for j in range(1, FEATS):
                total = total + urecv[side, t, j].astype(F32)
            resid = rown[t] - weight * total
            rown[t] = resid
            rt[t] = resid.astype(BF16)

        for q in range(4):
            w_copies[q].wait()
            for c in range(8 * q, 8 * q + 8):
                x_copies[c].wait()

            def start_block(g, carry, q=q):
                part = None
                for j in range(4):
                    c = 8 * q + 4 * g + j
                    prod = jnp.dot(xv[c], wst[c].astype(BF16), preferred_element_type=F32)
                    part = prod if part is None else part + prod
                uacc[...] = uacc[...] + part
                return carry

            if q == 0:
                uacc[...] = jnp.zeros_like(uacc)
            lax.fori_loop(0, 2, start_block, 0)
        for xq in range(4):
            cols = uacc[pl.ds(xq * LANES, LANES), :].T
            for t in range(STREAMS):
                ub[t, :, pl.ds(xq * LANES, LANES)] = cols[t * tgt:(t + 1) * tgt].astype(BF16)
        pl.semaphore_wait(barrier, 6 + FEATS - 1)
        for t in range(STREAMS):
            blocks_send(t, 0)
        eta_copy.wait()
        lam_copy.wait()
        lam_cols = jnp.broadcast_to(lam_ref[...], (LANES, LANES)).T
        for t in range(STREAMS):
            lamb[t] = lam_cols[t * tgt:(t + 1) * tgt]
        y_copy.wait()
        for xq in range(4):
            cols = yst[pl.ds(xq * LANES, LANES), :].T
            for t in range(STREAMS):
                rown[t, :, pl.ds(xq * LANES, LANES)] = cols[t * tgt:(t + 1) * tgt]
        for h in range(2):
            for pm in range(2):
                cols = wst[samp * 2 + h, pl.ds(pm * LANES, LANES), :].T
                for t in range(STREAMS):
                    wown[t, h, pm] = cols[t * tgt:(t + 1) * tgt]

        def turn(c, carry):
            xt[c] = xv[c].T
            return carry

        lax.fori_loop(0, 32, turn, 0)
        residual(0, 0, 1.0)

        rounds = STREAMS * SWEEPS

        def one_pass(i, carry):
            ta, tb, tc, td = (lax.rem(i + off, STREAMS) for off in (2, 1, 0, 3))
            in_a = (i >= 2) & (i < 2 + rounds)
            in_b = (i >= 3) & (i < 3 + rounds)
            in_c = (i >= STREAMS) & (i < STREAMS + rounds)
            in_d = i >= 1 + STREAMS
            wrap_up = i >= 3 + rounds - STREAMS
            side = lax.rem((i - 1) // STREAMS, 2)
            weight = jnp.where(i <= STREAMS, 1.0, STEP_WEIGHT).astype(F32)

            @pl.when(in_a)
            def _():
                slopes(ta, 2)

            @pl.when(in_b)
            def _():
                sum_second(tb)

            @pl.when(in_d)
            def _():
                gather_close(td, step_net)
                products(td, 2)
                blocks_out(td, side)

            @pl.when(in_c)
            def _():
                gather_second(tc, step_net)

            @pl.when(i > 2 + rounds - STREAMS + 2)
            def _():
                gather_third(td, coef_net)

            @pl.when((i > 2 + rounds - STREAMS + 1) & in_c)
            def _():
                gather_second(tc, coef_net)

            @pl.when(in_a)
            def _():
                slopes(ta, 1, 3, 0)

            @pl.when(in_a)
            def _():
                sum_first(ta)

            @pl.when(in_c)
            def _():
                products(tc, 0)

            @pl.when(in_c)
            def _():
                gather_third(tc, step_net)

            @pl.when(in_b)
            def _():
                take_step(tb)
                gather_open(tb, step_net)

            @pl.when(in_b & wrap_up)
            def _():
                coef_open(tb)

            @pl.when(in_c)
            def _():
                products(tc, -1)
                products(tc, 1)

            residual(td, side, weight)
            return carry

        lax.fori_loop(2, rounds + STREAMS + 1, one_pass, 0)

        r_done = pltpu.make_async_copy(rown, r_out, ysem)
        r_done.start()
        w_done = [pltpu.make_async_copy(wg.at[t], w_out.at[t], wsem.at[t]) for t in range(STREAMS)]
        for t in range(STREAMS):
            gather_close(t, coef_net)
            w_done[t].start()
        for t in range(STREAMS):
            w_done[t].wait()
        r_done.wait()

    return kernel


def solution(mesh):
    samp_size = mesh.shape["samp"]
    design_spec = P(("problem", "samp"), "feat")
    rows_spec = P(("problem", "samp"), None)
    coef_spec = P(("problem", "feat"), None)
    step_spec = P(("problem", "feat"))
    ridge_spec = P("problem")

    def local(design, targets, coef_init, step_sizes, ridge_weights):
        rows, cols = design.shape
        n_tgt = targets.shape[1]
        tgt = n_tgt // STREAMS
        half = tgt // 2
        own = (STREAMS, RING, RING, 2, tgt, 256)
        vm = pltpu.VMEM
        dma = pltpu.SemaphoreType.DMA
        any_spec = pl.BlockSpec(memory_space=pl.ANY)
        w_t, r_t = pl.pallas_call(
            make_kernel(rows * samp_size, tgt),
            out_shape=(jax.ShapeDtypeStruct(own, F32), jax.ShapeDtypeStruct((STREAMS, tgt, rows), F32)),
            in_specs=[any_spec] * 5,
            out_specs=(any_spec, any_spec),
            scratch_shapes=[
                vm((cols // LANES, LANES), F32),
                vm((1, n_tgt), F32),
                vm((32, rows, 256), BF16),
                vm((32, 256, rows), BF16),
                vm((32, 256, LANES), F32),
                vm((rows, LANES), F32),
                vm((rows, n_tgt), F32),
                vm(own, BF16),
                vm(own, F32),
                vm((STREAMS, 2, RING, 2, RING, tgt, LANES), F32),
                vm((STREAMS, 2, 2, RING, tgt, LANES), F32),
                vm((STREAMS, 2, 2, RING, tgt, LANES), F32),
                vm((STREAMS, 2, 2, RING, tgt, LANES), F32),
                vm((STREAMS, 2, 3, 2, tgt, LANES), F32),
                vm((STREAMS, 2, 2, tgt, LANES), F32),
                vm((STREAMS, tgt, LANES), F32),
                vm((STREAMS, tgt, rows), BF16),
                vm((STREAMS, tgt, rows), F32),
                vm((STREAMS, tgt, rows), BF16),
                vm((2, STREAMS, FEATS, tgt, rows), BF16),
                vm((STREAMS, tgt, rows), F32),
                dma((32,)),
                dma((4,)),
                dma((2,)),
                dma,
                dma((STREAMS, 2 * AG_MSGS)),
                dma((STREAMS, RS_MSGS)),
                dma((STREAMS, 2 * AG_MSGS)),
                dma((STREAMS, 2 * AG_MSGS)),
                dma((STREAMS, 2 * AG_MSGS)),
                dma((STREAMS, FEATS)),
                dma((2, STREAMS, FEATS)),
            ],
            compiler_params=pltpu.CompilerParams(collective_id=0, has_side_effects=True, vmem_limit_bytes=60 * 1024 * 1024),
        )(design, targets, coef_init.reshape(32, 256, n_tgt), step_sizes.reshape(cols // LANES, LANES), ridge_weights.reshape(1, n_tgt))
        coef, resid = pl.pallas_call(
            flip_results,
            in_specs=[any_spec, any_spec],
            out_specs=(any_spec, any_spec),
            out_shape=(jax.ShapeDtypeStruct((cols, n_tgt), F32), jax.ShapeDtypeStruct((rows, n_tgt), F32)),
            scratch_shapes=[
                vm((8, STREAMS, 2, 2, tgt, 256), F32),
                vm((STREAMS, tgt, rows), F32),
                vm((8, cols // 8, n_tgt), F32),
                vm((rows, n_tgt), F32),
                dma((8,)),
                dma((8,)),
                dma((2,)),
            ],
        )(w_t, r_t)
        return coef, resid

    return jax.shard_map(local, mesh=mesh, in_specs=(design_spec, rows_spec, coef_spec, step_spec, ridge_spec), out_specs=(coef_spec, rows_spec), check_vma=False)
```

```python
import jax
import jax.numpy as jnp
from jax import lax
from jax.experimental import pallas as pl
from jax.experimental.pallas import tpu as pltpu
from jax.sharding import PartitionSpec as P

SWEEPS = 4
STEP_WEIGHT = 0.5
RING = 4
FEATS = 8
LANES = 128
ORDER = (2, 1, 3, 0)
STREAMS = 4
MESH_ID = pl.DeviceIdType.MESH
AG_MSGS = 19
RS_MSGS = 26
F32 = jnp.float32
BF16 = jnp.bfloat16


def flip_results(w_hbm, r_hbm, coef_hbm, resid_hbm, w_in, r_in, coef, resid, in_sem, out_sem, r_sem):
    loads = [pltpu.make_async_copy(w_hbm.at[:, p // 2, pl.ds(p % 2 * 2, 2)], w_in.at[p], in_sem.at[p]) for p in range(8)]
    stores = [pltpu.make_async_copy(coef.at[p], coef_hbm.at[pl.ds(p * 1024, 1024)], out_sem.at[p]) for p in range(8)]
    r_load = pltpu.make_async_copy(r_hbm, r_in, r_sem.at[0])
    r_store = pltpu.make_async_copy(resid, resid_hbm, r_sem.at[1])
    r_load.start()
    for load in loads:
        load.start()
    r_load.wait()
    for xq in range(4):
        cols = [r_in[t, :, pl.ds(xq * LANES, LANES)] for t in range(STREAMS)]
        resid[pl.ds(xq * LANES, LANES), :] = jnp.concatenate(cols, axis=0).T
    r_store.start()
    for p in range(8):
        loads[p].wait()
        for y in range(2):
            for h in range(2):
                cols = [w_in[p, t, y, h] for t in range(STREAMS)]
                coef[p, pl.ds((y * 2 + h) * 256, 256), :] = jnp.concatenate(cols, axis=0).T
        stores[p].start()
    for p in range(8):
        stores[p].wait()
    r_store.wait()


def make_kernel(total_rows, tgt):
    half = tgt // 2
    inv_rows = 1.0 / total_rows

    def kernel(x_hbm, y_hbm, w0_hbm, eta_hbm, lam_hbm, w_out, r_out,
               eta_ref, lam_ref, xv, xt, wst, yst, uacc, sg, wg, gt, fin, din, cin, r2in, wown, lamb, rt, acc,
               ub, urecv, rown,
               xsem, wsem, psem, ysem, rs_send, rs_recv, ag_recv, w_send, w_recv, x_send, u_recv):
        samp = lax.axis_index("samp")
        feat = lax.axis_index("feat")
        zpos = samp // RING
        ypos = samp % RING

        def wrap(v):
            return lax.rem(v + RING, RING)

        def dev(z, y):
            return (0, z * RING + y, feat)

        z_plus, z_minus = dev(wrap(zpos + 1), ypos), dev(wrap(zpos - 1), ypos)
        y_plus, y_minus = dev(zpos, wrap(ypos + 1)), dev(zpos, wrap(ypos - 1))
        first_nbr = ((y_plus, y_minus), (z_plus, z_minus))
        second_nbr = ((z_plus, z_minus), (y_plus, y_minus))

        def place(h, o1, o2):
            if h == 0:
                return wrap(zpos + o2), wrap(ypos + o1)
            return wrap(zpos + o1), wrap(ypos + o2)

        def peer(k):
            return lax.rem(feat + k, FEATS)

        x_copies = [pltpu.make_async_copy(x_hbm.at[:, pl.ds(c * 256, 256)], xv.at[c], xsem.at[c]) for c in range(32)]
        w_copies = [pltpu.make_async_copy(w0_hbm.at[pl.ds(8 * q, 8)], wst.at[pl.ds(8 * q, 8)], wsem.at[q]) for q in range(4)]
        y_copy = pltpu.make_async_copy(y_hbm, yst, ysem)
        eta_copy = pltpu.make_async_copy(eta_hbm, eta_ref, psem.at[0])
        lam_copy = pltpu.make_async_copy(lam_hbm, lam_ref, psem.at[1])
        for q in range(4):
            w_copies[q].start()
            for c in range(8 * q, 8 * q + 8):
                x_copies[c].start()

        y_copy.start()
        eta_copy.start()
        lam_copy.start()

        barrier = pltpu.get_barrier_semaphore()
        for nbr in (z_plus, z_minus, y_plus, y_minus, dev(wrap(zpos + 2), ypos), dev(zpos, wrap(ypos + 2))):
            pl.semaphore_signal(barrier, inc=1, device_id=nbr, device_id_type=MESH_ID)
        for k in range(1, FEATS):
            pl.semaphore_signal(barrier, inc=1, device_id=(0, samp, peer(k)), device_id_type=MESH_ID)

        def remote(src, dst, send, recv, to):
            return pltpu.make_async_remote_copy(src_ref=src, dst_ref=dst, send_sem=send, recv_sem=recv, device_id=to, device_id_type=MESH_ID)

        def rs1(t, h, kind, way, part):
            io, pm = {"F": (2, way), "D": (1 + 2 * way, 1 - way), "C": (1 + 2 * way, way)}[kind]
            land = {"F": fin, "D": din, "C": cin}[kind]
            rows = pl.ds(0, 4) if kind == "D" else pl.ds(2 * part, 2)
            slot = (h * 2 + way) * 5 + {"F": part, "C": 2 + part, "D": 4}[kind]
            return remote(gt.at[t, h, io, pm, rows], land.at[t, h, way, rows], rs_send.at[t, slot], rs_recv.at[t, slot], first_nbr[h][way])

        def rs2(t, h, js):
            jo = ORDER[js]
            slot = 20 + h * 3 + js
            zi, yi = place(h, 0, jo)
            return remote(gt.at[t, h, 0, :, js], r2in.at[t, h, js], rs_send.at[t, slot], rs_recv.at[t, slot], dev(zi, yi))

        def ag(t, h, idx, buf, send, recv):
            if idx < 3:
                (o1, o2), rows = (0, 0), None
                to = dev(*place(h, 0, ORDER[idx]))
            elif idx < 11:
                way, m = (idx - 3) // 4, (idx - 3) % 4
                to, o1, rows = first_nbr[h][way], 0, None
                o2 = (0, -1, 1, 2)[m]
            else:
                way, m = (idx - 11) // 4, (idx - 11) % 4
                to, o1, rows = first_nbr[h][way], (-1, 1)[way], way
                o2 = (0, -1, 1, 2)[m]
            zi, yi = place(h, o1, o2)
            ref = buf.at[t, zi, yi, h] if rows is None else buf.at[t, zi, yi, h, pl.ds(rows * half, half)]
            slot = h * AG_MSGS + idx
            return remote(ref, ref, send.at[t, slot], recv.at[t, slot], to)

        def go(t, h, net, *idxs):
            for idx in idxs:
                ag(t, h, idx, *net).start()

        def got(t, h, net, *idxs):
            for idx in idxs:
                ag(t, h, idx, *net).wait_recv()

        step_net = (sg, rs_send, ag_recv)
        coef_net = (wg, w_send, w_recv)

        def gather_open(t, net):
            for h in range(2):
                go(t, h, net, 1, 2, 0, 3, 7)

        def gather_second(t, net):
            for h in range(2):
                got(t, h, net, 1)
                go(t, h, net, 4, 8)
                got(t, h, net, 2)
                go(t, h, net, 5, 9)
            for h in range(2):
                got(t, h, net, 0)
                go(t, h, net, 6, 10)
            for h in range(2):
                got(t, h, net, 3)
                go(t, h, net, 11)
                got(t, h, net, 7)
                go(t, h, net, 15)

        def gather_third(t, net):
            for h in range(2):
                for m in range(1, 4):
                    got(t, h, net, 3 + m)
                    go(t, h, net, 11 + m)
                    got(t, h, net, 7 + m)
                    go(t, h, net, 15 + m)

        def gather_close(t, net):
            for h in range(2):
                got(t, h, net, *range(11, 19))
            for h in range(2):
                for idx in range(AG_MSGS):
                    ag(t, h, idx, *net).wait_send()

        def slopes(t, *ios):
            for io in ios:
                for h in range(2):
                    for js in range(RING):
                        zi, yi = place(h, io, ORDER[js])
                        res = jnp.dot(rt[t], xv[(zi * RING + yi) * 2 + h], preferred_element_type=F32)
                        gt[t, h, io, 0, js] = res[:, :LANES]
                        gt[t, h, io, 1, js] = res[:, LANES:]
            for io in ios:
                for h in range(2):
                    if io == 2:
                        for part in range(2):
                            rs1(t, h, "F", 0, part).start()
                            rs1(t, h, "F", 1, part).start()
                    elif io:
                        rs1(t, h, "D", io // 2, 0).start()

        def sum_first(t):
            for part in range(2):
                rows = pl.ds(2 * part, 2)
                for h in range(2):
                    for way in range(2):
                        rs1(t, h, "F", way, part).wait_recv()
                        gt[t, h, 1 + 2 * way, way, rows] += fin[t, h, way, rows]
                        rs1(t, h, "C", way, part).start()

        def sum_second(t):
            for part in range(2):
                for h in range(2):
                    for way in range(2):
                        if part == 0:
                            rs1(t, h, "D", way, 0).wait_recv()
                        rs1(t, h, "C", way, part).wait_recv()
                    for js in range(2 * part, 2 * part + 2):
                        for pm in range(2):
                            gt[t, h, 0, pm, js] = gt[t, h, 0, pm, js] + cin[t, h, pm, js] + din[t, h, 1 - pm, js]
                        if js < 3:
                            rs2(t, h, js).start()

        def take_step(t):
            for h in range(2):
                for js in range(3):
                    rs2(t, h, js).wait_recv()
                for pm in range(2):
                    grad = (gt[t, h, 0, pm, 3] + r2in[t, h, 0, pm] + r2in[t, h, 1, pm] + r2in[t, h, 2, pm]) * inv_rows
                    old = wown[t, h, pm]
                    step = eta_ref[pl.ds((samp * 2 + h) * 2 + pm, 1), :] * (grad - lamb[t] * old)
                    wown[t, h, pm] = old + STEP_WEIGHT * step
                    sg[t, zpos, ypos, h, :, pl.ds(pm * LANES, LANES)] = step.astype(BF16)
            for h in range(2):
                for way in range(2):
                    rs1(t, h, "D", way, 0).wait_send()
                    for part in range(2):
                        rs1(t, h, "F", way, part).wait_send()
                        rs1(t, h, "C", way, part).wait_send()
                for js in range(3):
                    rs2(t, h, js).wait_send()

        def coef_open(t):
            for h in range(2):
                for pm in range(2):
                    wg[t, zpos, ypos, h, :, pl.ds(pm * LANES, LANES)] = wown[t, h, pm]
            gather_open(t, coef_net)

        def products(t, o1):
            part = None
            for h in range(2):
                for o2 in (0, -1, 1, 2):
                    zi, yi = place(h, o1, o2)
                    c = (zi * RING + yi) * 2 + h
                    prod = jnp.dot(sg[t, zi, yi, h], xt[c], preferred_element_type=F32)
                    part = prod if part is None else part + prod
            acc[t] = part if o1 == 0 else acc[t] + part

        def umsg(t, k, side):
            return remote(ub.at[t], urecv.at[side, t, feat], x_send.at[t, k], u_recv.at[side, t, k], (0, samp, peer(k)))

        def blocks_send(t, side):
            for k in range(1, FEATS):
                umsg(t, k, side).start()
            urecv[side, t, feat] = ub[t]

        def blocks_out(t, side):
            ub[t] = acc[t].astype(BF16)
            blocks_send(t, side)

        def residual(t, side, weight):
            for k in range(1, FEATS):
                umsg(t, k, side).wait()
            total = urecv[side, t, 0].astype(F32)
            for j in range(1, FEATS):
                total = total + urecv[side, t, j].astype(F32)
            resid = rown[t] - weight * total
            rown[t] = resid
            rt[t] = resid.astype(BF16)

        for q in range(4):
            w_copies[q].wait()
            for c in range(8 * q, 8 * q + 8):
                x_copies[c].wait()

            def start_block(g, carry, q=q):
                part = None
                for j in range(4):
                    c = 8 * q + 4 * g + j
                    prod = jnp.dot(xv[c], wst[c].astype(BF16), preferred_element_type=F32)
                    part = prod if part is None else part + prod
                uacc[...] = uacc[...] + part
                return carry

            if q == 0:
                uacc[...] = jnp.zeros_like(uacc)
            lax.fori_loop(0, 2, start_block, 0)
        for xq in range(4):
            cols = uacc[pl.ds(xq * LANES, LANES), :].T
            for t in range(STREAMS):
                ub[t, :, pl.ds(xq * LANES, LANES)] = cols[t * tgt:(t + 1) * tgt].astype(BF16)
        pl.semaphore_wait(barrier, 6 + FEATS - 1)
        for t in range(STREAMS):
            blocks_send(t, 0)
        eta_copy.wait()
        lam_copy.wait()
        lam_cols = jnp.broadcast_to(lam_ref[...], (LANES, LANES)).T
        for t in range(STREAMS):
            lamb[t] = lam_cols[t * tgt:(t + 1) * tgt]
        y_copy.wait()
        for xq in range(4):
            cols = yst[pl.ds(xq * LANES, LANES), :].T
            for t in range(STREAMS):
                rown[t, :, pl.ds(xq * LANES, LANES)] = cols[t * tgt:(t + 1) * tgt]
        for h in range(2):
            for pm in range(2):
                cols = wst[samp * 2 + h, pl.ds(pm * LANES, LANES), :].T
                for t in range(STREAMS):
                    wown[t, h, pm] = cols[t * tgt:(t + 1) * tgt]

        def turn(c, carry):
            xt[c] = xv[c].T
            return carry

        lax.fori_loop(0, 32, turn, 0)
        residual(0, 0, 1.0)

        rounds = STREAMS * SWEEPS

        def one_pass(i, carry):
            ta, tb, tc, td = (lax.rem(i + off, STREAMS) for off in (2, 1, 0, 3))
            in_a = (i >= 2) & (i < 2 + rounds)
            in_b = (i >= 3) & (i < 3 + rounds)
            in_c = (i >= STREAMS) & (i < STREAMS + rounds)
            in_d = i >= 1 + STREAMS
            wrap_up = i >= 3 + rounds - STREAMS
            side = lax.rem((i - 1) // STREAMS, 2)
            weight = jnp.where(i <= STREAMS, 1.0, STEP_WEIGHT).astype(F32)

            @pl.when(in_a)
            def _():
                slopes(ta, 2)

            @pl.when(in_b)
            def _():
                sum_second(tb)

            @pl.when(in_d)
            def _():
                gather_close(td, step_net)
                products(td, 2)
                blocks_out(td, side)

            @pl.when(in_c)
            def _():
                gather_second(tc, step_net)

            @pl.when(i > 2 + rounds - STREAMS + 2)
            def _():
                gather_third(td, coef_net)

            @pl.when((i > 2 + rounds - STREAMS + 1) & in_c)
            def _():
                gather_second(tc, coef_net)

            @pl.when(in_a)
            def _():
                slopes(ta, 1, 3, 0)

            @pl.when(in_a)
            def _():
                sum_first(ta)

            @pl.when(in_c)
            def _():
                products(tc, 0)

            @pl.when(in_c)
            def _():
                gather_third(tc, step_net)

            @pl.when(in_c)
            def _():
                products(tc, 1)

            @pl.when(in_b)
            def _():
                take_step(tb)
                gather_open(tb, step_net)

            @pl.when(in_b & wrap_up)
            def _():
                coef_open(tb)

            @pl.when(in_c)
            def _():
                products(tc, -1)

            residual(td, side, weight)

            return carry

        lax.fori_loop(2, rounds + STREAMS + 1, one_pass, 0)

        r_done = pltpu.make_async_copy(rown, r_out, ysem)
        r_done.start()
        w_done = [pltpu.make_async_copy(wg.at[t], w_out.at[t], wsem.at[t]) for t in range(STREAMS)]
        for t in range(STREAMS):
            gather_close(t, coef_net)
            w_done[t].start()
        for t in range(STREAMS):
            w_done[t].wait()
        r_done.wait()

    return kernel


def solution(mesh):
    samp_size = mesh.shape["samp"]
    design_spec = P(("problem", "samp"), "feat")
    rows_spec = P(("problem", "samp"), None)
    coef_spec = P(("problem", "feat"), None)
    step_spec = P(("problem", "feat"))
    ridge_spec = P("problem")

    def local(design, targets, coef_init, step_sizes, ridge_weights):
        rows, cols = design.shape
        n_tgt = targets.shape[1]
        tgt = n_tgt // STREAMS
        half = tgt // 2
        own = (STREAMS, RING, RING, 2, tgt, 256)
        vm = pltpu.VMEM
        dma = pltpu.SemaphoreType.DMA
        any_spec = pl.BlockSpec(memory_space=pl.ANY)
        w_t, r_t = pl.pallas_call(
            make_kernel(rows * samp_size, tgt),
            out_shape=(jax.ShapeDtypeStruct(own, F32), jax.ShapeDtypeStruct((STREAMS, tgt, rows), F32)),
            in_specs=[any_spec] * 5,
            out_specs=(any_spec, any_spec),
            scratch_shapes=[
                vm((cols // LANES, LANES), F32),
                vm((1, n_tgt), F32),
                vm((32, rows, 256), BF16),
                vm((32, 256, rows), BF16),
                vm((32, 256, LANES), F32),
                vm((rows, LANES), F32),
                vm((rows, n_tgt), F32),
                vm(own, BF16),
                vm(own, F32),
                vm((STREAMS, 2, RING, 2, RING, tgt, LANES), F32),
                vm((STREAMS, 2, 2, RING, tgt, LANES), F32),
                vm((STREAMS, 2, 2, RING, tgt, LANES), F32),
                vm((STREAMS, 2, 2, RING, tgt, LANES), F32),
                vm((STREAMS, 2, 3, 2, tgt, LANES), F32),
                vm((STREAMS, 2, 2, tgt, LANES), F32),
                vm((STREAMS, tgt, LANES), F32),
                vm((STREAMS, tgt, rows), BF16),
                vm((STREAMS, tgt, rows), F32),
                vm((STREAMS, tgt, rows), BF16),
                vm((2, STREAMS, FEATS, tgt, rows), BF16),
                vm((STREAMS, tgt, rows), F32),
                dma((32,)),
                dma((4,)),
                dma((2,)),
                dma,
                dma((STREAMS, 2 * AG_MSGS)),
                dma((STREAMS, RS_MSGS)),
                dma((STREAMS, 2 * AG_MSGS)),
                dma((STREAMS, 2 * AG_MSGS)),
                dma((STREAMS, 2 * AG_MSGS)),
                dma((STREAMS, FEATS)),
                dma((2, STREAMS, FEATS)),
            ],
            compiler_params=pltpu.CompilerParams(collective_id=0, has_side_effects=True, vmem_limit_bytes=60 * 1024 * 1024),
        )(design, targets, coef_init.reshape(32, 256, n_tgt), step_sizes.reshape(cols // LANES, LANES), ridge_weights.reshape(1, n_tgt))
        coef, resid = pl.pallas_call(
            flip_results,
            in_specs=[any_spec, any_spec],
            out_specs=(any_spec, any_spec),
            out_shape=(jax.ShapeDtypeStruct((cols, n_tgt), F32), jax.ShapeDtypeStruct((rows, n_tgt), F32)),
            scratch_shapes=[
                vm((8, STREAMS, 2, 2, tgt, 256), F32),
                vm((STREAMS, tgt, rows), F32),
                vm((8, cols // 8, n_tgt), F32),
                vm((rows, n_tgt), F32),
                dma((8,)),
                dma((8,)),
                dma((2,)),
            ],
        )(w_t, r_t)
        return coef, resid

    return jax.shard_map(local, mesh=mesh, in_specs=(design_spec, rows_spec, coef_spec, step_spec, ridge_spec), out_specs=(coef_spec, rows_spec), check_vma=False)
```

```python
import jax
import jax.numpy as jnp
from jax import lax
from jax.experimental import pallas as pl
from jax.experimental.pallas import tpu as pltpu
from jax.sharding import PartitionSpec as P

SWEEPS = 4
STEP_WEIGHT = 0.5
RING = 4
FEATS = 8
LANES = 128
ORDER = (2, 1, 3, 0)
STREAMS = 4
MESH_ID = pl.DeviceIdType.MESH
AG_MSGS = 19
RS_MSGS = 26
F32 = jnp.float32
BF16 = jnp.bfloat16


def flip_results(w_hbm, r_hbm, coef_hbm, resid_hbm, w_in, r_in, coef, resid, in_sem, out_sem, r_sem):
    loads = [pltpu.make_async_copy(w_hbm.at[:, p // 2, pl.ds(p % 2 * 2, 2)], w_in.at[p], in_sem.at[p]) for p in range(8)]
    stores = [pltpu.make_async_copy(coef.at[p], coef_hbm.at[pl.ds(p * 1024, 1024)], out_sem.at[p]) for p in range(8)]
    r_load = pltpu.make_async_copy(r_hbm, r_in, r_sem.at[0])
    r_store = pltpu.make_async_copy(resid, resid_hbm, r_sem.at[1])
    r_load.start()
    for load in loads:
        load.start()
    r_load.wait()
    for xq in range(4):
        cols = [r_in[t, :, pl.ds(xq * LANES, LANES)] for t in range(STREAMS)]
        resid[pl.ds(xq * LANES, LANES), :] = jnp.concatenate(cols, axis=0).T
    r_store.start()
    for p in range(8):
        loads[p].wait()
        for y in range(2):
            for h in range(2):
                cols = [w_in[p, t, y, h] for t in range(STREAMS)]
                coef[p, pl.ds((y * 2 + h) * 256, 256), :] = jnp.concatenate(cols, axis=0).T
        stores[p].start()
    for p in range(8):
        stores[p].wait()
    r_store.wait()


def make_kernel(total_rows, tgt):
    half = tgt // 2
    inv_rows = 1.0 / total_rows

    def kernel(x_hbm, y_hbm, w0_hbm, eta_hbm, lam_hbm, w_out, r_out,
               eta_ref, lam_ref, xv, xt, wst, yst, uacc, sg, wg, gt, fin, din, cin, r2in, wown, lamb, rt, acc,
               ub, urecv, rown,
               xsem, wsem, psem, ysem, rs_send, rs_recv, ag_recv, w_send, w_recv, x_send, u_recv):
        samp = lax.axis_index("samp")
        feat = lax.axis_index("feat")
        zpos = samp // RING
        ypos = samp % RING

        def wrap(v):
            return lax.rem(v + RING, RING)

        def dev(z, y):
            return (0, z * RING + y, feat)

        z_plus, z_minus = dev(wrap(zpos + 1), ypos), dev(wrap(zpos - 1), ypos)
        y_plus, y_minus = dev(zpos, wrap(ypos + 1)), dev(zpos, wrap(ypos - 1))
        first_nbr = ((y_plus, y_minus), (z_plus, z_minus))
        second_nbr = ((z_plus, z_minus), (y_plus, y_minus))

        def place(h, o1, o2):
            if h == 0:
                return wrap(zpos + o2), wrap(ypos + o1)
            return wrap(zpos + o1), wrap(ypos + o2)

        def peer(k):
            return lax.rem(feat + k, FEATS)

        x_copies = [pltpu.make_async_copy(x_hbm.at[:, pl.ds(c * 256, 256)], xv.at[c], xsem.at[c]) for c in range(32)]
        w_copies = [pltpu.make_async_copy(w0_hbm.at[pl.ds(8 * q, 8)], wst.at[pl.ds(8 * q, 8)], wsem.at[q]) for q in range(4)]
        y_copy = pltpu.make_async_copy(y_hbm, yst, ysem)
        eta_copy = pltpu.make_async_copy(eta_hbm, eta_ref, psem.at[0])
        lam_copy = pltpu.make_async_copy(lam_hbm, lam_ref, psem.at[1])
        for q in range(4):
            w_copies[q].start()
            for c in range(8 * q, 8 * q + 8):
                x_copies[c].start()

        y_copy.start()
        eta_copy.start()
        lam_copy.start()

        barrier = pltpu.get_barrier_semaphore()
        for nbr in (z_plus, z_minus, y_plus, y_minus, dev(wrap(zpos + 2), ypos), dev(zpos, wrap(ypos + 2))):
            pl.semaphore_signal(barrier, inc=1, device_id=nbr, device_id_type=MESH_ID)
        for k in range(1, FEATS):
            pl.semaphore_signal(barrier, inc=1, device_id=(0, samp, peer(k)), device_id_type=MESH_ID)

        def remote(src, dst, send, recv, to):
            return pltpu.make_async_remote_copy(src_ref=src, dst_ref=dst, send_sem=send, recv_sem=recv, device_id=to, device_id_type=MESH_ID)

        def rs1(t, h, kind, way, part):
            io, pm = {"F": (2, way), "D": (1 + 2 * way, 1 - way), "C": (1 + 2 * way, way)}[kind]
            land = {"F": fin, "D": din, "C": cin}[kind]
            rows = pl.ds(0, 4) if kind == "D" else pl.ds(2 * part, 2)
            slot = (h * 2 + way) * 5 + {"F": part, "C": 2 + part, "D": 4}[kind]
            return remote(gt.at[t, h, io, pm, rows], land.at[t, h, way, rows], rs_send.at[t, slot], rs_recv.at[t, slot], first_nbr[h][way])

        def rs2(t, h, js):
            jo = ORDER[js]
            slot = 20 + h * 3 + js
            zi, yi = place(h, 0, jo)
            return remote(gt.at[t, h, 0, :, js], r2in.at[t, h, js], rs_send.at[t, slot], rs_recv.at[t, slot], dev(zi, yi))

        def ag(t, h, idx, buf, send, recv):
            if idx < 3:
                (o1, o2), rows = (0, 0), None
                to = dev(*place(h, 0, ORDER[idx]))
            elif idx < 11:
                way, m = (idx - 3) // 4, (idx - 3) % 4
                to, o1, rows = first_nbr[h][way], 0, None
                o2 = (0, -1, 1, 2)[m]
            else:
                way, m = (idx - 11) // 4, (idx - 11) % 4
                to, o1, rows = first_nbr[h][way], (-1, 1)[way], way
                o2 = (0, -1, 1, 2)[m]
            zi, yi = place(h, o1, o2)
            ref = buf.at[t, zi, yi, h] if rows is None else buf.at[t, zi, yi, h, pl.ds(rows * half, half)]
            slot = h * AG_MSGS + idx
            return remote(ref, ref, send.at[t, slot], recv.at[t, slot], to)

        def go(t, h, net, *idxs):
            for idx in idxs:
                ag(t, h, idx, *net).start()

        def got(t, h, net, *idxs):
            for idx in idxs:
                ag(t, h, idx, *net).wait_recv()

        step_net = (sg, rs_send, ag_recv)
        coef_net = (wg, w_send, w_recv)

        def gather_open(t, net):
            for h in range(2):
                go(t, h, net, 1, 2, 0, 3, 7)

        def gather_second(t, net):
            for h in range(2):
                got(t, h, net, 1)
                go(t, h, net, 4, 8)
                got(t, h, net, 2)
                go(t, h, net, 5, 9)
            for h in range(2):
                got(t, h, net, 0)
                go(t, h, net, 6, 10)
            for h in range(2):
                got(t, h, net, 3)
                go(t, h, net, 11)
                got(t, h, net, 7)
                go(t, h, net, 15)

        def gather_third(t, net):
            for h in range(2):
                for m in range(1, 4):
                    got(t, h, net, 3 + m)
                    go(t, h, net, 11 + m)
                    got(t, h, net, 7 + m)
                    go(t, h, net, 15 + m)

        def gather_close(t, net):
            for h in range(2):
                got(t, h, net, *range(11, 19))
            for h in range(2):
                for idx in range(AG_MSGS):
                    ag(t, h, idx, *net).wait_send()

        def slopes(t, *ios):
            for io in ios:
                for h in range(2):
                    for js in range(RING):
                        zi, yi = place(h, io, ORDER[js])
                        res = jnp.dot(rt[t], xv[(zi * RING + yi) * 2 + h], preferred_element_type=F32)
                        gt[t, h, io, 0, js] = res[:, :LANES]
                        gt[t, h, io, 1, js] = res[:, LANES:]
                    if io == 2:
                        for part in range(2):
                            rs1(t, h, "F", 0, part).start()
                            rs1(t, h, "F", 1, part).start()
            for io in ios:
                for h in range(2):
                    if io % 2:
                        rs1(t, h, "D", io // 2, 0).start()

        def sum_first(t):
            for part in range(2):
                rows = pl.ds(2 * part, 2)
                for h in range(2):
                    for way in range(2):
                        rs1(t, h, "F", way, part).wait_recv()
                        gt[t, h, 1 + 2 * way, way, rows] += fin[t, h, way, rows]
                        rs1(t, h, "C", way, part).start()

        def sum_second(t):
            for part in range(2):
                for h in range(2):
                    for way in range(2):
                        if part == 0:
                            rs1(t, h, "D", way, 0).wait_recv()
                        rs1(t, h, "C", way, part).wait_recv()
                    for js in range(2 * part, 2 * part + 2):
                        for pm in range(2):
                            gt[t, h, 0, pm, js] = gt[t, h, 0, pm, js] + cin[t, h, pm, js] + din[t, h, 1 - pm, js]
                        if js < 3:
                            rs2(t, h, js).start()

        def take_step(t):
            for h in range(2):
                for js in range(3):
                    rs2(t, h, js).wait_recv()
                for pm in range(2):
                    grad = (gt[t, h, 0, pm, 3] + r2in[t, h, 0, pm] + r2in[t, h, 1, pm] + r2in[t, h, 2, pm]) * inv_rows
                    old = wown[t, h, pm]
                    step = eta_ref[pl.ds((samp * 2 + h) * 2 + pm, 1), :] * (grad - lamb[t] * old)
                    wown[t, h, pm] = old + STEP_WEIGHT * step
                    sg[t, zpos, ypos, h, :, pl.ds(pm * LANES, LANES)] = step.astype(BF16)
            for h in range(2):
                for way in range(2):
                    rs1(t, h, "D", way, 0).wait_send()
                    for part in range(2):
                        rs1(t, h, "F", way, part).wait_send()
                        rs1(t, h, "C", way, part).wait_send()
                for js in range(3):
                    rs2(t, h, js).wait_send()

        def coef_open(t):
            for h in range(2):
                for pm in range(2):
                    wg[t, zpos, ypos, h, :, pl.ds(pm * LANES, LANES)] = wown[t, h, pm]
            gather_open(t, coef_net)

        def products(t, o1):
            part = None
            for h in range(2):
                for o2 in (0, -1, 1, 2):
                    zi, yi = place(h, o1, o2)
                    c = (zi * RING + yi) * 2 + h
                    prod = jnp.dot(sg[t, zi, yi, h], xt[c], preferred_element_type=F32)
                    part = prod if part is None else part + prod
            acc[t] = part if o1 == 0 else acc[t] + part

        def umsg(t, k, side):
            return remote(ub.at[t], urecv.at[side, t, feat], x_send.at[t, k], u_recv.at[side, t, k], (0, samp, peer(k)))

        def blocks_send(t, side):
            for k in range(1, FEATS):
                umsg(t, k, side).start()
            urecv[side, t, feat] = ub[t]

        def blocks_out(t, side):
            ub[t] = acc[t].astype(BF16)
            blocks_send(t, side)

        def residual(t, side, weight):
            for k in range(1, FEATS):
                umsg(t, k, side).wait()
            total = urecv[side, t, 0].astype(F32)
            for j in range(1, FEATS):
                total = total + urecv[side, t, j].astype(F32)
            resid = rown[t] - weight * total
            rown[t] = resid
            rt[t] = resid.astype(BF16)

        for q in range(4):
            w_copies[q].wait()
            for c in range(8 * q, 8 * q + 8):
                x_copies[c].wait()

            def start_block(g, carry, q=q):
                part = None
                for j in range(4):
                    c = 8 * q + 4 * g + j
                    prod = jnp.dot(xv[c], wst[c].astype(BF16), preferred_element_type=F32)
                    part = prod if part is None else part + prod
                uacc[...] = uacc[...] + part
                return carry

            if q == 0:
                uacc[...] = jnp.zeros_like(uacc)
            lax.fori_loop(0, 2, start_block, 0)
        for xq in range(4):
            cols = uacc[pl.ds(xq * LANES, LANES), :].T
            for t in range(STREAMS):
                ub[t, :, pl.ds(xq * LANES, LANES)] = cols[t * tgt:(t + 1) * tgt].astype(BF16)
        pl.semaphore_wait(barrier, 6 + FEATS - 1)
        for t in range(STREAMS):
            blocks_send(t, 0)
        eta_copy.wait()
        lam_copy.wait()
        lam_cols = jnp.broadcast_to(lam_ref[...], (LANES, LANES)).T
        for t in range(STREAMS):
            lamb[t] = lam_cols[t * tgt:(t + 1) * tgt]
        y_copy.wait()
        for xq in range(4):
            cols = yst[pl.ds(xq * LANES, LANES), :].T
            for t in range(STREAMS):
                rown[t, :, pl.ds(xq * LANES, LANES)] = cols[t * tgt:(t + 1) * tgt]
        for h in range(2):
            for pm in range(2):
                cols = wst[samp * 2 + h, pl.ds(pm * LANES, LANES), :].T
                for t in range(STREAMS):
                    wown[t, h, pm] = cols[t * tgt:(t + 1) * tgt]

        def turn(c, carry):
            xt[c] = xv[c].T
            return carry

        lax.fori_loop(0, 32, turn, 0)
        residual(0, 0, 1.0)

        rounds = STREAMS * SWEEPS

        def one_pass(i, carry):
            ta, tb, tc, td = (lax.rem(i + off, STREAMS) for off in (2, 1, 0, 3))
            in_a = (i >= 2) & (i < 2 + rounds)
            in_b = (i >= 3) & (i < 3 + rounds)
            in_c = (i >= STREAMS) & (i < STREAMS + rounds)
            in_d = i >= 1 + STREAMS
            wrap_up = i >= 3 + rounds - STREAMS
            side = lax.rem((i - 1) // STREAMS, 2)
            weight = jnp.where(i <= STREAMS, 1.0, STEP_WEIGHT).astype(F32)

            @pl.when(in_a)
            def _():
                slopes(ta, 2)

            @pl.when(in_b)
            def _():
                sum_second(tb)

            @pl.when(in_d)
            def _():
                gather_close(td, step_net)
                products(td, 2)
                blocks_out(td, side)

            @pl.when(in_c)
            def _():
                gather_second(tc, step_net)

            @pl.when(i > 2 + rounds - STREAMS + 2)
            def _():
                gather_third(td, coef_net)

            @pl.when((i > 2 + rounds - STREAMS + 1) & in_c)
            def _():
                gather_second(tc, coef_net)

            @pl.when(in_a)
            def _():
                slopes(ta, 1, 3, 0)

            @pl.when(in_a)
            def _():
                sum_first(ta)

            @pl.when(in_c)
            def _():
                products(tc, 0)

            @pl.when(in_c)
            def _():
                gather_third(tc, step_net)

            @pl.when(in_c)
            def _():
                products(tc, 1)

            @pl.when(in_b)
            def _():
                take_step(tb)
                gather_open(tb, step_net)

            @pl.when(in_b & wrap_up)
            def _():
                coef_open(tb)

            @pl.when(in_c)
            def _():
                products(tc, -1)

            residual(td, side, weight)

            return carry

        lax.fori_loop(2, rounds + STREAMS + 1, one_pass, 0)

        r_done = pltpu.make_async_copy(rown, r_out, ysem)
        r_done.start()
        w_done = [pltpu.make_async_copy(wg.at[t], w_out.at[t], wsem.at[t]) for t in range(STREAMS)]
        for t in range(STREAMS):
            gather_close(t, coef_net)
            w_done[t].start()
        for t in range(STREAMS):
            w_done[t].wait()
        r_done.wait()

    return kernel


def solution(mesh):
    samp_size = mesh.shape["samp"]
    design_spec = P(("problem", "samp"), "feat")
    rows_spec = P(("problem", "samp"), None)
    coef_spec = P(("problem", "feat"), None)
    step_spec = P(("problem", "feat"))
    ridge_spec = P("problem")

    def local(design, targets, coef_init, step_sizes, ridge_weights):
        rows, cols = design.shape
        n_tgt = targets.shape[1]
        tgt = n_tgt // STREAMS
        half = tgt // 2
        own = (STREAMS, RING, RING, 2, tgt, 256)
        vm = pltpu.VMEM
        dma = pltpu.SemaphoreType.DMA
        any_spec = pl.BlockSpec(memory_space=pl.ANY)
        w_t, r_t = pl.pallas_call(
            make_kernel(rows * samp_size, tgt),
            out_shape=(jax.ShapeDtypeStruct(own, F32), jax.ShapeDtypeStruct((STREAMS, tgt, rows), F32)),
            in_specs=[any_spec] * 5,
            out_specs=(any_spec, any_spec),
            scratch_shapes=[
                vm((cols // LANES, LANES), F32),
                vm((1, n_tgt), F32),
                vm((32, rows, 256), BF16),
                vm((32, 256, rows), BF16),
                vm((32, 256, LANES), F32),
                vm((rows, LANES), F32),
                vm((rows, n_tgt), F32),
                vm(own, BF16),
                vm(own, F32),
                vm((STREAMS, 2, RING, 2, RING, tgt, LANES), F32),
                vm((STREAMS, 2, 2, RING, tgt, LANES), F32),
                vm((STREAMS, 2, 2, RING, tgt, LANES), F32),
                vm((STREAMS, 2, 2, RING, tgt, LANES), F32),
                vm((STREAMS, 2, 3, 2, tgt, LANES), F32),
                vm((STREAMS, 2, 2, tgt, LANES), F32),
                vm((STREAMS, tgt, LANES), F32),
                vm((STREAMS, tgt, rows), BF16),
                vm((STREAMS, tgt, rows), F32),
                vm((STREAMS, tgt, rows), BF16),
                vm((2, STREAMS, FEATS, tgt, rows), BF16),
                vm((STREAMS, tgt, rows), F32),
                dma((32,)),
                dma((4,)),
                dma((2,)),
                dma,
                dma((STREAMS, 2 * AG_MSGS)),
                dma((STREAMS, RS_MSGS)),
                dma((STREAMS, 2 * AG_MSGS)),
                dma((STREAMS, 2 * AG_MSGS)),
                dma((STREAMS, 2 * AG_MSGS)),
                dma((STREAMS, FEATS)),
                dma((2, STREAMS, FEATS)),
            ],
            compiler_params=pltpu.CompilerParams(collective_id=0, has_side_effects=True, vmem_limit_bytes=60 * 1024 * 1024),
        )(design, targets, coef_init.reshape(32, 256, n_tgt), step_sizes.reshape(cols // LANES, LANES), ridge_weights.reshape(1, n_tgt))
        coef, resid = pl.pallas_call(
            flip_results,
            in_specs=[any_spec, any_spec],
            out_specs=(any_spec, any_spec),
            out_shape=(jax.ShapeDtypeStruct((cols, n_tgt), F32), jax.ShapeDtypeStruct((rows, n_tgt), F32)),
            scratch_shapes=[
                vm((8, STREAMS, 2, 2, tgt, 256), F32),
                vm((STREAMS, tgt, rows), F32),
                vm((8, cols // 8, n_tgt), F32),
                vm((rows, n_tgt), F32),
                dma((8,)),
                dma((8,)),
                dma((2,)),
            ],
        )(w_t, r_t)
        return coef, resid

    return jax.shard_map(local, mesh=mesh, in_specs=(design_spec, rows_spec, coef_spec, step_spec, ridge_spec), out_specs=(coef_spec, rows_spec), check_vma=False)
```
